32 devices in a mesh: agg: 2 (over y), gx: 4 (over x, core), gy: 4 (over z).
Axes of the slice: x: 2, y: 2, z: 4, core: 2. Of those that a mesh axis runs over, the one named last changes fastest.
Arguments:
- velocity_prev: float32 [3, 32, 64, 256], P(None, 'gx', 'gy', 'agg'), may hold values from -6 to 6
- forcing: float32 [3, 32, 64, 256], P(None, 'gx', 'gy', 'agg'), may hold values from -6 to 6
- reaction: float32 [32, 64, 256], P('gx', 'gy', 'agg'), may hold values from 0.1 to 4
Outputs:
- velocity: float32 [3, 32, 64, 256], P(None, 'gx', 'gy', 'agg')
- compressed: float32 [3, 64, 256, 16], P(None, 'gy', ('agg', 'gx'))
The draws below stay inside these ranges and needn't reach their ends.
All inputs are finite; a program needn't handle non-finite values.
Results may differ from the reference program's by a relative error of at most 0.00002.
Values sent between devices are 32-bit elements; how exact they have to be, the bound alone decides.
A program may use at most 64 MiB of HBM per device.

```python
import math
import jax
import jax.numpy as jnp
from jax import lax

SWEEPS = 2
COARSE_SWEEPS = 4
LX = 5
NX = 32
NY = 64
NZ = 256


def shard_levels(rng, dims, cuts, low, top_value):
    loudness, own = 1.0, jax.random.fold_in(rng, 6)
    for axis_at, blocks in cuts:
        heights = jnp.exp(jax.random.uniform(jax.random.fold_in(own, axis_at), (blocks,), jnp.float32, low / len(cuts), top_value / len(cuts)))
        loudness = loudness * jnp.repeat(heights, dims[axis_at] // blocks).reshape([-1 if axis == axis_at else 1 for axis in range(len(dims))])
    return loudness


def normal_values(key, shape, scale, limit, split=(), kind=jnp.bfloat16):
    result = jax.random.normal(key, shape, jnp.float32) * scale
    if len(split) > 0:
        result = shard_levels(key, shape, split, -0.22, 0.18) * result
    return jnp.clip(result, min=-limit, max=limit).astype(kind)


def setup_inputs(seed: int = 0) -> dict:
    key_list = jax.random.split(jax.random.key(seed), 4)
    velocity_prev = normal_values(key_list[0], (3, NX, NY, NZ), 1.0, 6.0, ((1, 4), (2, 4), (3, 2)), jnp.float32)
    forcing = normal_values(key_list[1], (3, NX, NY, NZ), 1.0, 6.0, ((1, 4), (2, 4), (3, 2)), jnp.float32)
    reaction = jnp.clip(jnp.exp(math.log(4.0) - 3.6888794 * jax.random.uniform(key_list[2], (NX, NY, NZ), jnp.float32) ** shard_levels(key_list[2], (NX, NY, NZ), ((0, 4), (1, 4), (2, 2)), -0.2, 0.2)), 0.1, 4.0)
    return dict(velocity_prev=velocity_prev, forcing=forcing, reaction=reaction)


damping = 0.8
root_half = 0.7071067811865476


def neighbours(field):
    padded = jnp.pad(field, 1)
    summed = padded[2:, 1:-1, 1:-1] + padded[:-2, 1:-1, 1:-1]
    summed = summed + padded[1:-1, 2:, 1:-1] + padded[1:-1, :-2, 1:-1]
    summed = summed + padded[1:-1, 1:-1, 2:] + padded[1:-1, 1:-1, :-2]
    return summed


def fine_residual(current, forcing_part, diagonal):
    return forcing_part - (diagonal * current - neighbours(current))


def block_mean(field):
    size_x, size_y, size_z = field.shape
    return field.reshape(size_x // 2, 2, size_y // 2, 2, size_z // 2, 2).mean(axis=(1, 3, 5))


def prolong(coarse):
    size_x, size_y, size_z = coarse.shape
    expanded = jnp.broadcast_to(coarse[:, None, :, None, :, None], (size_x, 2, size_y, 2, size_z, 2))
    return expanded.reshape(2 * size_x, 2 * size_y, 2 * size_z)


def halve_last(values):
    paired = values.reshape(values.shape[:-1] + (values.shape[-1] // 2, 2))
    even_cells = paired[..., 0]
    odd_cells = paired[..., 1]
    return (even_cells + odd_cells) * root_half, (even_cells - odd_cells) * root_half


def x_levels(approx):
    details = []
    for level_index in range(LX - 1):
        approx, detail = halve_last(approx)
        details.append(detail)
    return jnp.concatenate([approx] + details[::-1], axis=-1)


def pair_pass(values, which_dim):
    layout = values.shape
    paired = values.reshape(layout[:which_dim] + (layout[which_dim] // 2, 2) + layout[which_dim + 1:])
    even_cells = lax.index_in_dim(paired, 0, which_dim + 1, keepdims=False)
    odd_cells = lax.index_in_dim(paired, 1, which_dim + 1, keepdims=False)
    stacked = jnp.stack([(even_cells + odd_cells) * root_half, (even_cells - odd_cells) * root_half], axis=which_dim + 1)
    return stacked.reshape(layout)


def reference(velocity_prev, forcing, reaction):
    diagonal = 6.0 + reaction
    coarse_diag = (6.0 + 4.0 * block_mean(reaction)) * 0.25

    def solve_component(inputs):
        previous, forcing_part = inputs
        current = previous
        for sweep_index in range(SWEEPS):
            current = current + damping * fine_residual(current, forcing_part, diagonal) / diagonal
        coarse_rhs = block_mean(fine_residual(current, forcing_part, diagonal))
        correction = damping * coarse_rhs / coarse_diag
        for sweep_index in range(COARSE_SWEEPS - 1):
            correction = correction + damping * (coarse_rhs - (coarse_diag * correction - 0.25 * neighbours(correction))) / coarse_diag
        current = current + prolong(correction)
        current = current + damping * fine_residual(current, forcing_part, diagonal) / diagonal
        x_lines = jnp.transpose(previous, (1, 2, 0))
        coeffs = x_levels(halve_last(x_lines)[0])
        coeffs = pair_pass(pair_pass(coeffs, 0), 1)
        return current, coeffs

    velocity, compressed = lax.map(solve_component, (velocity_prev, forcing))
    return velocity, compressed
```

```python
import functools

import jax
import jax.numpy as jnp
import numpy as np
from jax import lax
from jax.experimental import pallas as pl
from jax.experimental.pallas import tpu as pltpu
from jax.sharding import PartitionSpec as P

SWEEPS = 2
COARSE_SWEEPS = 4
LX = 5
MESH = pl.DeviceIdType.MESH

damping = 0.8
keep = 1.0 - damping
root_half = 0.7071067811865476


def local_levels(cells_x):
    return min(LX, cells_x.bit_length() - 1)


def finish_matrix(cells_x, blocks, rows):
    levels = local_levels(cells_x)
    kept = cells_x // 2
    eye = np.eye(blocks * kept).reshape(blocks, kept, blocks * kept)
    width = cells_x >> levels
    approx = eye[:, :width].reshape(blocks * width, -1)
    details, at = [], width
    for level in range(levels, 1, -1):
        width = cells_x >> level
        details.append(eye[:, at : at + width].reshape(blocks * width, -1))
        at += width
    for level in range(levels, LX):
        low, high = approx[0::2], approx[1::2]
        approx, detail = (low + high) * root_half, (low - high) * root_half
        details.insert(0, detail)
    along_x = np.concatenate([approx] + details, axis=0)
    along_y = np.zeros((rows, rows))
    for row in range(0, rows, 2):
        along_y[row, row : row + 2] = root_half
        along_y[row + 1, row : row + 2] = root_half, -root_half
    return np.einsum("qk,yr->kryq", along_x, along_y).reshape(blocks * kept * rows, -1).astype(np.float32)


def neighbour_sides():
    return [(axis, high) for axis in ("gx", "gy", "agg") for high in (False, True)]


def kernel(
    sizes, v_ref, f_ref, r_ref, m_ref, vel_ref, comp_ref,
    xs_fine, xr_fine, ys_fine, yr_fine, zs_fine, zr_fine,
    xs_coarse, xr_coarse, ys_coarse, yr_coarse, zs_coarse, zr_coarse,
    c_send, c_recv, w_buf, send_sem, recv_sem, c_send_sem, c_recv_sem,
):
    counts = sizes
    C, X, Y, Z = v_ref.shape
    Xc = X // 2
    half = Z // 2
    me = {axis: lax.axis_index(axis) for axis in counts}
    blocks = counts["gx"]
    chunk = Z // blocks

    def exists(axis, high):
        return me[axis] < counts[axis] - 1 if high else me[axis] > 0

    barrier = pltpu.get_barrier_semaphore()
    expected = blocks - 1
    for step in range(1, blocks):
        pl.semaphore_signal(
            barrier, inc=1, device_id={"gx": lax.rem(me["gx"] + step, blocks)}, device_id_type=MESH
        )
    for axis, high in neighbour_sides()[2:]:
        there = exists(axis, high)
        expected = expected + there.astype(jnp.int32)

        @pl.when(there)
        def _():
            pl.semaphore_signal(
                barrier, inc=1, device_id={axis: me[axis] + (1 if high else -1)}, device_id_type=MESH
            )

    received = {"gx": (xr_fine, xr_coarse), "gy": (yr_fine, yr_coarse), "agg": (zr_fine, zr_coarse)}
    for axis, high in neighbour_sides():
        @pl.when(jnp.logical_not(exists(axis, high)))
        def _():
            for buffer in received[axis]:
                for phase in range(buffer.shape[0]):
                    buffer[phase, int(high)] = jnp.zeros(buffer.shape[2:], buffer.dtype)

    row = lax.broadcasted_iota(jnp.int32, (Y, Z), 0)
    lane = lax.broadcasted_iota(jnp.int32, (Y, Z), 1)
    zero = jnp.zeros((Y, Z), jnp.float32)

    def pack(fields, width, phase, xs, ys, zs, store_x):
        if store_x:
            for c in range(C):
                xs[phase, 0, c] = fields[c][0]
                xs[phase, 1, c] = fields[c][width - 1]
        packed = zero
        for c in range(C):
            for x in range(width):
                k = c * width + x
                field = fields[c][x]
                ys[phase, 0, k : k + 1] = field[0:1]
                ys[phase, 1, k : k + 1] = field[Y - 1 : Y]
                packed = jnp.where(lane == k, field[:, 0:1], packed)
                packed = jnp.where(lane == half + k, field[:, Z - 1 : Z], packed)
        zs[phase] = packed

    def copies(fine, phase):
        number = phase if fine else SWEEPS + 1 + phase
        xs, xr, ys, yr, zs, zr = (
            (xs_fine, xr_fine, ys_fine, yr_fine, zs_fine, zr_fine)
            if fine
            else (xs_coarse, xr_coarse, ys_coarse, yr_coarse, zs_coarse, zr_coarse)
        )
        made = []
        for slot, (axis, high) in enumerate(neighbour_sides()):
            side = int(high)
            if axis == "gx":
                if fine and phase == 0:
                    src = v_ref.at[:, X - 1 if high else 0]
                else:
                    src = xs.at[phase, side]
                dst = xr.at[phase, 1 - side]
            elif axis == "gy":
                src, dst = ys.at[phase, side], yr.at[phase, 1 - side]
            else:
                src, dst = zs.at[phase], zr.at[phase, 1 - side]
            made.append((
                axis,
                high,
                pltpu.make_async_remote_copy(
                    src_ref=src,
                    dst_ref=dst,
                    send_sem=send_sem.at[number, slot],
                    recv_sem=recv_sem.at[number, slot],
                    device_id={axis: me[axis] + (1 if high else -1)},
                    device_id_type=MESH,
                ),
            ))
        return made

    def start(fine, phase):
        for axis, high, copy in copies(fine, phase):
            pl.when(exists(axis, high))(copy.start)

    def arrive(fine, phase):
        for axis, high, copy in copies(fine, phase):
            pl.when(exists(axis, not high))(copy.wait_recv)

    def sent(fine, phase):
        for axis, high, copy in copies(fine, phase):
            pl.when(exists(axis, high))(copy.wait_send)

    def inner_sum(fields, width, stride):
        sums = []
        for c in range(C):
            line = []
            for x in range(width):
                field = fields[c][x]
                total = jnp.where(row < stride, zero, pltpu.roll(field, stride, 0))
                total = total + jnp.where(row >= Y - stride, zero, pltpu.roll(field, Y - stride, 0))
                total = total + jnp.where(lane < stride, zero, pltpu.roll(field, stride, 1))
                total = total + jnp.where(lane >= Z - stride, zero, pltpu.roll(field, Z - stride, 1))
                if x > 0:
                    total = total + fields[c][x - 1]
                if x < width - 1:
                    total = total + fields[c][x + 1]
                line.append(total)
            sums.append(line)
        return sums

    def outer_sum(sums, width, stride, phase, xr, yr, zr, repeat=1):
        from_low, from_high = zr[phase, 0], zr[phase, 1]
        result = []
        for c in range(C):
            line = []
            for x in range(width):
                k = c * (width // repeat) + x // repeat
                total = sums[c][x]
                total = total + jnp.where(row < stride, yr[phase, 0, k : k + 1], 0.0)
                total = total + jnp.where(row >= Y - stride, yr[phase, 1, k : k + 1], 0.0)
                total = total + jnp.where(lane < stride, from_low[:, half + k : half + k + 1], 0.0)
                total = total + jnp.where(lane >= Z - stride, from_high[:, k : k + 1], 0.0)
                if x == 0:
                    total = total + xr[phase, 0, c]
                if x == width - 1:
                    total = total + xr[phase, 1, c]
                line.append(total)
            result.append(line)
        return result

    fine_recv = (xr_fine, yr_fine, zr_fine)
    coarse_recv = (xr_coarse, yr_coarse, zr_coarse)
    fine_send = (xs_fine, ys_fine, zs_fine)
    coarse_send = (xs_coarse, ys_coarse, zs_coarse)

    previous = [[v_ref[c, x] for x in range(X)] for c in range(C)]
    pack(previous, X, 0, *fine_send, False)
    pl.semaphore_wait(barrier, expected)
    start(True, 0)

    kept = X // 2
    levels = local_levels(X)
    even_row = row % 2 == 0
    even_lane = lane % 2 == 0
    combos_per_tile = Z // chunk
    coefficients = []
    for c in range(C):
        approx, details = previous[c], []
        for level in range(levels):
            low, high = approx[0::2], approx[1::2]
            approx = [(a + b) * root_half for a, b in zip(low, high)]
            if level > 0:
                details = [(a - b) * root_half for a, b in zip(low, high)] + details
        line = []
        for field in approx + details:
            swapped = jnp.where(even_lane, pltpu.roll(field, Z - 1, 1), pltpu.roll(field, 1, 1))
            line.append((jnp.where(even_lane, field, -field) + swapped) * root_half)
        coefficients.append(line)
    row8 = lax.broadcasted_iota(jnp.int32, (8, Z), 1)
    parts = Y // 8
    for j in range(blocks):
        for k in range(kept):
            tiles = {}
            for c in range(C):
                for part in range(parts):
                    tile, place = divmod(c * parts + part, combos_per_tile)
                    field = coefficients[c][k][part * 8 : part * 8 + 8]
                    shift = (place * chunk - j * chunk) % Z
                    moved = pltpu.roll(field, shift, 1) if shift else field
                    if tile in tiles:
                        moved = jnp.where((row8 >= place * chunk) & (row8 < (place + 1) * chunk), moved, tiles[tile])
                    tiles[tile] = moved
            for tile, value in tiles.items():
                c_send[j, tile, k] = value

    def c_copy(j, source):
        return pltpu.make_async_remote_copy(
            src_ref=c_send.at[j],
            dst_ref=c_recv.at[source],
            send_sem=c_send_sem.at[j],
            recv_sem=c_recv_sem.at[source],
            device_id={"gx": j},
            device_id_type=MESH,
        )

    for j in range(blocks):
        pl.when(me["gx"] != j)(c_copy(j, me["gx"]).start)

        @pl.when(me["gx"] == j)
        def _():
            c_recv[j] = c_send[j]

    def finish_compressed():
        for j in range(blocks):
            pl.when(me["gx"] != j)(c_copy(j, j).wait_recv)
        coefs = blocks * kept
        for tile in range(c_send.shape[1]):
            gathered = c_recv[:, tile].reshape(coefs * 8, Z)
            done = lax.dot_general(
                gathered, m_ref[...], (((0,), (0,)), ((), ())),
                precision=lax.Precision.HIGHEST, preferred_element_type=jnp.float32,
            )
            for place in range(combos_per_tile):
                c, part = divmod(tile * combos_per_tile + place, parts)
                if c < C:
                    for y in range(8):
                        comp_ref[c, part * 8 + y] = done[
                            place * chunk : (place + 1) * chunk, y * coefs : (y + 1) * coefs
                        ]

    diagonal = [6.0 + r_ref[x] for x in range(X)]
    for x in range(X):
        w_buf[x] = damping / diagonal[x]
    field = previous
    for sweep in range(SWEEPS):
        sums = inner_sum(field, X, 1)
        sums = [[sums[c][x] + f_ref[c, x] for x in range(X)] for c in range(C)]
        arrive(True, sweep)
        sums = outer_sum(sums, X, 1, sweep, *fine_recv)
        field = [[keep * field[c][x] + w_buf[x] * sums[c][x] for x in range(X)] for c in range(C)]
        pack(field, X, sweep + 1, *fine_send, True)
        start(True, sweep + 1)

    def pooled(planes):
        out = []
        for x in range(0, len(planes), 2):
            total = planes[x] + planes[x + 1]
            total = total + jnp.where(even_row, pltpu.roll(total, Y - 1, 0), pltpu.roll(total, 1, 0))
            total = total + jnp.where(even_lane, pltpu.roll(total, Z - 1, 1), pltpu.roll(total, 1, 1))
            out.append(total * 0.125)
        return out

    sums = inner_sum(field, X, 1)
    sums = [[sums[c][x] + f_ref[c, x] for x in range(X)] for c in range(C)]
    coarse_weight = [damping / ((6.0 + 4.0 * mean) * 0.25) for mean in pooled([r_ref[x] for x in range(X)])]
    arrive(True, SWEEPS)
    sums = outer_sum(sums, X, 1, SWEEPS, *fine_recv)
    coarse_rhs = [
        pooled([sums[c][x] - (6.0 + r_ref[x]) * field[c][x] for x in range(X)]) for c in range(C)
    ]
    correction = [[coarse_weight[x] * coarse_rhs[c][x] for x in range(Xc)] for c in range(C)]
    pack(correction, Xc, 0, *coarse_send, True)
    start(False, 0)
    finish_compressed()
    for step in range(COARSE_SWEEPS - 1):
        coarse_sums = inner_sum(correction, Xc, 2)
        arrive(False, step)
        coarse_sums = outer_sum(coarse_sums, Xc, 2, step, *coarse_recv)
        correction = [
            [
                keep * correction[c][x] + coarse_weight[x] * (coarse_rhs[c][x] + 0.25 * coarse_sums[c][x])
                for x in range(Xc)
            ]
            for c in range(C)
        ]
        pack(correction, Xc, step + 1, *coarse_send, True)
        start(False, step + 1)
    spread = [[correction[c][x // 2] for x in range(X)] for c in range(C)]
    added = inner_sum(spread, X, 1)
    sums = [[sums[c][x] + added[c][x] for x in range(X)] for c in range(C)]
    arrive(False, COARSE_SWEEPS - 1)
    sums = outer_sum(sums, X, 1, COARSE_SWEEPS - 1, *coarse_recv, repeat=2)
    for c in range(C):
        for x in range(X):
            vel_ref[c, x] = keep * (field[c][x] + spread[c][x]) + w_buf[x] * sums[c][x]

    for phase in range(SWEEPS + 1):
        sent(True, phase)
    for phase in range(COARSE_SWEEPS):
        sent(False, phase)
    for j in range(blocks):
        pl.when(me["gx"] != j)(c_copy(j, me["gx"]).wait_send)


def on_device(counts, velocity_prev, forcing, reaction):
    C, X, Y, Z = velocity_prev.shape
    blocks = counts["gx"]
    kept = X // 2
    chunk = Z // blocks
    tiles = -(-(C * (Y // 8)) // (Z // chunk))
    matrix = jnp.asarray(finish_matrix(X, blocks, 8))
    vmem = pl.BlockSpec(memory_space=pltpu.VMEM)

    def buffers(phases, width):
        return [
            pltpu.VMEM((phases, 2, C, Y, Z), jnp.float32),
            pltpu.VMEM((phases, 2, C, Y, Z), jnp.float32),
            pltpu.VMEM((phases, 2, C * width, Z), jnp.float32),
            pltpu.VMEM((phases, 2, C * width, Z), jnp.float32),
            pltpu.VMEM((phases, Y, Z), jnp.float32),
            pltpu.VMEM((phases, 2, Y, Z), jnp.float32),
        ]

    phases = SWEEPS + 1 + COARSE_SWEEPS
    return pl.pallas_call(
        functools.partial(kernel, counts),
        out_shape=(
            jax.ShapeDtypeStruct((C, X, Y, Z), jnp.float32),
            jax.ShapeDtypeStruct((C, Y, chunk, kept * blocks), jnp.float32),
        ),
        in_specs=[vmem] * 4,
        out_specs=(vmem, vmem),
        scratch_shapes=buffers(SWEEPS + 1, X) + buffers(COARSE_SWEEPS, X // 2) + [
            pltpu.VMEM((blocks, tiles, kept, 8, Z), jnp.float32),
            pltpu.VMEM((blocks, tiles, kept, 8, Z), jnp.float32),
            pltpu.VMEM((X, Y, Z), jnp.float32),
            pltpu.SemaphoreType.DMA((phases, 6)),
            pltpu.SemaphoreType.DMA((phases, 6)),
            pltpu.SemaphoreType.DMA((blocks,)),
            pltpu.SemaphoreType.DMA((blocks,)),
        ],
        compiler_params=pltpu.CompilerParams(collective_id=0, has_side_effects=True),
    )(velocity_prev, forcing, reaction, matrix)


def solution(mesh):
    counts = {axis: mesh.shape[axis] for axis in ("agg", "gx", "gy")}
    placed = (P(None, "gx", "gy", "agg"), P(None, "gx", "gy", "agg"), P("gx", "gy", "agg"))
    return jax.shard_map(
        functools.partial(on_device, counts),
        mesh=mesh,
        in_specs=placed,
        out_specs=(P(None, "gx", "gy", "agg"), P(None, "gy", ("agg", "gx"), None)),
        check_vma=False,
    )
```

```python
import functools

import jax
import jax.numpy as jnp
import numpy as np
from jax import lax
from jax.experimental import pallas as pl
from jax.experimental.pallas import tpu as pltpu
from jax.sharding import PartitionSpec as P

SWEEPS = 2
COARSE_SWEEPS = 4
LX = 5
MESH = pl.DeviceIdType.MESH

damping = 0.8
keep = 1.0 - damping
root_half = 0.7071067811865476


def local_levels(cells_x):
    return min(LX, cells_x.bit_length() - 1)


def finish_matrix(cells_x, blocks, rows):
    levels = local_levels(cells_x)
    kept = cells_x // 2
    eye = np.eye(blocks * kept).reshape(blocks, kept, blocks * kept)
    width = cells_x >> levels
    approx = eye[:, :width].reshape(blocks * width, -1)
    details, at = [], width
    for level in range(levels, 1, -1):
        width = cells_x >> level
        details.append(eye[:, at : at + width].reshape(blocks * width, -1))
        at += width
    for level in range(levels, LX):
        low, high = approx[0::2], approx[1::2]
        approx, detail = (low + high) * root_half, (low - high) * root_half
        details.insert(0, detail)
    along_x = np.concatenate([approx] + details, axis=0)
    along_y = np.zeros((rows, rows))
    for row in range(0, rows, 2):
        along_y[row, row : row + 2] = root_half
        along_y[row + 1, row : row + 2] = root_half, -root_half
    return np.einsum("qk,yr->yqkr", along_x, along_y).reshape(-1, blocks * kept * rows).astype(np.float32)


def neighbour_sides():
    return [(axis, high) for axis in ("gx", "gy", "agg") for high in (False, True)]


def kernel(
    sizes, v_hbm, f_hbm, r_hbm, m_hbm, vel_ref, comp_ref, v_ref, f_ref, r_ref, m_ref,
    xs_fine, xr_fine, ys_fine, yr_fine, zs_fine, zr_fine,
    xs_coarse, xr_coarse, ys_coarse, yr_coarse, zs_coarse, zr_coarse,
    c_send, c_recv, w_buf, send_sem, recv_sem, c_send_sem, c_recv_sem, in_sem,
):
    counts = sizes
    C, X, Y, Z = v_ref.shape
    Xc = X // 2
    half = Z // 2
    me = {axis: lax.axis_index(axis) for axis in counts}
    blocks = counts["gx"]
    chunk = Z // blocks

    def exists(axis, high):
        return me[axis] < counts[axis] - 1 if high else me[axis] > 0

    loads = [
        pltpu.make_async_copy(src, dst, in_sem.at[i])
        for i, (src, dst) in enumerate(
            ((v_hbm, v_ref), (f_hbm, f_ref), (r_hbm, r_ref), (m_hbm, m_ref))
        )
    ]
    for load in loads:
        load.start()
    barrier = pltpu.get_barrier_semaphore()
    expected = blocks - 1
    for step in range(1, blocks):
        pl.semaphore_signal(
            barrier, inc=1, device_id={"gx": lax.rem(me["gx"] + step, blocks)}, device_id_type=MESH
        )
    for axis, high in neighbour_sides()[2:]:
        there = exists(axis, high)
        expected = expected + there.astype(jnp.int32)

        @pl.when(there)
        def _():
            pl.semaphore_signal(
                barrier, inc=1, device_id={axis: me[axis] + (1 if high else -1)}, device_id_type=MESH
            )

    received = {"gx": (xr_fine, xr_coarse), "gy": (yr_fine, yr_coarse), "agg": (zr_fine, zr_coarse)}
    for axis, high in neighbour_sides():
        @pl.when(jnp.logical_not(exists(axis, high)))
        def _():
            for buffer in received[axis]:
                for phase in range(buffer.shape[0]):
                    buffer[phase, int(high)] = jnp.zeros(buffer.shape[2:], buffer.dtype)

    row = lax.broadcasted_iota(jnp.int32, (Y, Z), 0)
    lane = lax.broadcasted_iota(jnp.int32, (Y, Z), 1)
    zero = jnp.zeros((Y, Z), jnp.float32)

    def pack(fields, width, phase, xs, ys, zs):
        packed = zero
        for c in range(C):
            for x in range(width):
                k = c * width + x
                field = fields[c][x]
                ys[phase, 0, k : k + 1] = field[0:1]
                ys[phase, 1, k : k + 1] = field[Y - 1 : Y]
                packed = jnp.where(lane == k, field[:, 0:1], packed)
                packed = jnp.where(lane == half + k, field[:, Z - 1 : Z], packed)
        zs[phase] = packed

    def copies(fine, phase):
        number = phase if fine else SWEEPS + 1 + phase
        xs, xr, ys, yr, zs, zr = (
            (xs_fine, xr_fine, ys_fine, yr_fine, zs_fine, zr_fine)
            if fine
            else (xs_coarse, xr_coarse, ys_coarse, yr_coarse, zs_coarse, zr_coarse)
        )
        made = []
        for slot, (axis, high) in enumerate(neighbour_sides()):
            side = int(high)
            if axis == "gx":
                if fine and phase == 0:
                    src = v_ref.at[:, X - 1 if high else 0]
                else:
                    src = xs.at[phase, side]
                dst = xr.at[phase, 1 - side]
            elif axis == "gy":
                src, dst = ys.at[phase, side], yr.at[phase, 1 - side]
            else:
                src, dst = zs.at[phase], zr.at[phase, 1 - side]
            made.append((
                axis,
                high,
                pltpu.make_async_remote_copy(
                    src_ref=src,
                    dst_ref=dst,
                    send_sem=send_sem.at[number, slot],
                    recv_sem=recv_sem.at[number, slot],
                    device_id={axis: me[axis] + (1 if high else -1)},
                    device_id_type=MESH,
                ),
            ))
        return made

    def start(fine, phase, axes=("gx", "gy", "agg")):
        for axis, high, copy in copies(fine, phase):
            if axis in axes:
                pl.when(exists(axis, high))(copy.start)

    def send(fine, phase, fields, width):
        xs, ys, zs = fine_send if fine else coarse_send
        for c in range(C):
            xs[phase, 0, c] = fields[c][0]
            xs[phase, 1, c] = fields[c][width - 1]
        start(fine, phase, ("gx",))
        pack(fields, width, phase, xs, ys, zs)
        start(fine, phase, ("gy", "agg"))

    def arrive(fine, phase):
        for axis, high, copy in copies(fine, phase):
            pl.when(exists(axis, not high))(copy.wait_recv)

    def sent(fine, phase):
        for axis, high, copy in copies(fine, phase):
            pl.when(exists(axis, high))(copy.wait_send)

    def inner_sum(fields, width, stride):
        sums = []
        for c in range(C):
            line = []
            for x in range(width):
                field = fields[c][x]
                total = jnp.where(row < stride, zero, pltpu.roll(field, stride, 0))
                total = total + jnp.where(row >= Y - stride, zero, pltpu.roll(field, Y - stride, 0))
                total = total + jnp.where(lane < stride, zero, pltpu.roll(field, stride, 1))
                total = total + jnp.where(lane >= Z - stride, zero, pltpu.roll(field, Z - stride, 1))
                if x > 0:
                    total = total + fields[c][x - 1]
                if x < width - 1:
                    total = total + fields[c][x + 1]
                line.append(total)
            sums.append(line)
        return sums

    def outer_sum(sums, width, stride, phase, xr, yr, zr, repeat=1):
        from_low, from_high = zr[phase, 0], zr[phase, 1]
        result = []
        for c in range(C):
            line = []
            for x in range(width):
                k = c * (width // repeat) + x // repeat
                total = sums[c][x]
                total = total + jnp.where(row < stride, yr[phase, 0, k : k + 1], 0.0)
                total = total + jnp.where(row >= Y - stride, yr[phase, 1, k : k + 1], 0.0)
                total = total + jnp.where(lane < stride, from_low[:, half + k : half + k + 1], 0.0)
                total = total + jnp.where(lane >= Z - stride, from_high[:, k : k + 1], 0.0)
                if x == 0:
                    total = total + xr[phase, 0, c]
                if x == width - 1:
                    total = total + xr[phase, 1, c]
                line.append(total)
            result.append(line)
        return result

    fine_recv = (xr_fine, yr_fine, zr_fine)
    coarse_recv = (xr_coarse, yr_coarse, zr_coarse)
    fine_send = (xs_fine, ys_fine, zs_fine)
    coarse_send = (xs_coarse, ys_coarse, zs_coarse)

    loads[0].wait()
    previous = [[v_ref[c, x] for x in range(X)] for c in range(C)]
    pack(previous, X, 0, *fine_send)
    pl.semaphore_wait(barrier, expected)
    start(True, 0)

    kept = X // 2
    levels = local_levels(X)
    even_row = row % 2 == 0
    even_lane = lane % 2 == 0
    combos_per_tile = Z // chunk
    coefficients = []
    for c in range(C):
        approx, details = previous[c], []
        for level in range(levels):
            low, high = approx[0::2], approx[1::2]
            approx = [(a + b) * root_half for a, b in zip(low, high)]
            if level > 0:
                details = [(a - b) * root_half for a, b in zip(low, high)] + details
        line = []
        for field in approx + details:
            swapped = jnp.where(even_lane, pltpu.roll(field, Z - 1, 1), pltpu.roll(field, 1, 1))
            line.append((jnp.where(even_lane, field, -field) + swapped) * root_half)
        coefficients.append(line)
    row8 = lax.broadcasted_iota(jnp.int32, (8, Z), 1)
    parts = Y // 8
    for j in range(blocks):
        for k in range(kept):
            tiles = {}
            for c in range(C):
                for part in range(parts):
                    tile, place = divmod(c * parts + part, combos_per_tile)
                    field = coefficients[c][k][part * 8 : part * 8 + 8]
                    shift = (place * chunk - j * chunk) % Z
                    moved = pltpu.roll(field, shift, 1) if shift else field
                    if tile in tiles:
                        moved = jnp.where((row8 >= place * chunk) & (row8 < (place + 1) * chunk), moved, tiles[tile])
                    tiles[tile] = moved
            for tile, value in tiles.items():
                c_send[j, tile, k] = value

    def c_copy(j, source):
        return pltpu.make_async_remote_copy(
            src_ref=c_send.at[j],
            dst_ref=c_recv.at[source],
            send_sem=c_send_sem.at[j],
            recv_sem=c_recv_sem.at[source],
            device_id={"gx": j},
            device_id_type=MESH,
        )

    for j in range(blocks):
        pl.when(me["gx"] != j)(c_copy(j, me["gx"]).start)

        @pl.when(me["gx"] == j)
        def _():
            c_recv[j] = c_send[j]

    def finish_compressed():
        for j in range(blocks):
            pl.when(me["gx"] != j)(c_copy(j, j).wait_recv)
        loads[3].wait()
        coefs = blocks * kept
        for tile in range(c_send.shape[1]):
            gathered = c_recv[:, tile].reshape(coefs * 8, Z)
            done = lax.dot_general(
                m_ref[...], gathered, (((1,), (0,)), ((), ())),
                precision=lax.Precision.HIGHEST, preferred_element_type=jnp.float32,
            )
            for place in range(combos_per_tile):
                c, part = divmod(tile * combos_per_tile + place, parts)
                if c < C:
                    for y in range(8):
                        comp_ref[c, part * 8 + y] = done[
                            y * coefs : (y + 1) * coefs, place * chunk : (place + 1) * chunk
                        ]

    loads[1].wait()
    loads[2].wait()
    diagonal = [6.0 + r_ref[x] for x in range(X)]
    for x in range(X):
        w_buf[x] = damping / diagonal[x]
    field = previous
    for sweep in range(SWEEPS):
        sums = inner_sum(field, X, 1)
        sums = [[sums[c][x] + f_ref[c, x] for x in range(X)] for c in range(C)]
        arrive(True, sweep)
        sums = outer_sum(sums, X, 1, sweep, *fine_recv)
        field = [[keep * field[c][x] + w_buf[x] * sums[c][x] for x in range(X)] for c in range(C)]
        send(True, sweep + 1, field, X)

    def pooled(planes):
        out = []
        for x in range(0, len(planes), 2):
            total = planes[x] + planes[x + 1]
            total = total + jnp.where(even_row, pltpu.roll(total, Y - 1, 0), pltpu.roll(total, 1, 0))
            total = total + jnp.where(even_lane, pltpu.roll(total, Z - 1, 1), pltpu.roll(total, 1, 1))
            out.append(total * 0.125)
        return out

    sums = inner_sum(field, X, 1)
    sums = [[sums[c][x] + f_ref[c, x] for x in range(X)] for c in range(C)]
    coarse_weight = [damping / ((6.0 + 4.0 * mean) * 0.25) for mean in pooled([r_ref[x] for x in range(X)])]
    arrive(True, SWEEPS)
    sums = outer_sum(sums, X, 1, SWEEPS, *fine_recv)
    coarse_rhs = [
        pooled([sums[c][x] - (6.0 + r_ref[x]) * field[c][x] for x in range(X)]) for c in range(C)
    ]
    correction = [[coarse_weight[x] * coarse_rhs[c][x] for x in range(Xc)] for c in range(C)]
    send(False, 0, correction, Xc)
    finish_compressed()
    for step in range(COARSE_SWEEPS - 1):
        coarse_sums = inner_sum(correction, Xc, 2)
        arrive(False, step)
        coarse_sums = outer_sum(coarse_sums, Xc, 2, step, *coarse_recv)
        correction = [
            [
                keep * correction[c][x] + coarse_weight[x] * (coarse_rhs[c][x] + 0.25 * coarse_sums[c][x])
                for x in range(Xc)
            ]
            for c in range(C)
        ]
        send(False, step + 1, correction, Xc)
    spread = [[correction[c][x // 2] for x in range(X)] for c in range(C)]
    added = inner_sum(spread, X, 1)
    sums = [[sums[c][x] + added[c][x] for x in range(X)] for c in range(C)]
    arrive(False, COARSE_SWEEPS - 1)
    sums = outer_sum(sums, X, 1, COARSE_SWEEPS - 1, *coarse_recv, repeat=2)
    for c in range(C):
        for x in range(X):
            vel_ref[c, x] = keep * (field[c][x] + spread[c][x]) + w_buf[x] * sums[c][x]

    for phase in range(SWEEPS + 1):
        sent(True, phase)
    for phase in range(COARSE_SWEEPS):
        sent(False, phase)
    for j in range(blocks):
        pl.when(me["gx"] != j)(c_copy(j, me["gx"]).wait_send)


def on_device(counts, velocity_prev, forcing, reaction):
    C, X, Y, Z = velocity_prev.shape
    blocks = counts["gx"]
    kept = X // 2
    chunk = Z // blocks
    tiles = -(-(C * (Y // 8)) // (Z // chunk))
    matrix = jnp.asarray(finish_matrix(X, blocks, 8))
    vmem = pl.BlockSpec(memory_space=pltpu.VMEM)

    def buffers(phases, width):
        return [
            pltpu.VMEM((phases, 2, C, Y, Z), jnp.float32),
            pltpu.VMEM((phases, 2, C, Y, Z), jnp.float32),
            pltpu.VMEM((phases, 2, C * width, Z), jnp.float32),
            pltpu.VMEM((phases, 2, C * width, Z), jnp.float32),
            pltpu.VMEM((phases, Y, Z), jnp.float32),
            pltpu.VMEM((phases, 2, Y, Z), jnp.float32),
        ]

    phases = SWEEPS + 1 + COARSE_SWEEPS
    velocity, compressed = pl.pallas_call(
        functools.partial(kernel, counts),
        out_shape=(
            jax.ShapeDtypeStruct((C, X, Y, Z), jnp.float32),
            jax.ShapeDtypeStruct((C, Y, kept * blocks, chunk), jnp.float32),
        ),
        in_specs=[pl.BlockSpec(memory_space=pltpu.HBM)] * 4,
        out_specs=(vmem, vmem),
        scratch_shapes=[
            pltpu.VMEM((C, X, Y, Z), jnp.float32),
            pltpu.VMEM((C, X, Y, Z), jnp.float32),
            pltpu.VMEM((X, Y, Z), jnp.float32),
            pltpu.VMEM(matrix.shape, jnp.float32),
        ] + buffers(SWEEPS + 1, X) + buffers(COARSE_SWEEPS, X // 2) + [
            pltpu.VMEM((blocks, tiles, kept, 8, Z), jnp.float32),
            pltpu.VMEM((blocks, tiles, kept, 8, Z), jnp.float32),
            pltpu.VMEM((X, Y, Z), jnp.float32),
            pltpu.SemaphoreType.DMA((phases, 6)),
            pltpu.SemaphoreType.DMA((phases, 6)),
            pltpu.SemaphoreType.DMA((blocks,)),
            pltpu.SemaphoreType.DMA((blocks,)),
            pltpu.SemaphoreType.DMA((4,)),
        ],
        compiler_params=pltpu.CompilerParams(collective_id=0, has_side_effects=True, vmem_limit_bytes=24 * 2**20),
    )(velocity_prev, forcing, reaction, matrix)
    return velocity, jnp.swapaxes(compressed, 2, 3)


def solution(mesh):
    counts = {axis: mesh.shape[axis] for axis in ("agg", "gx", "gy")}
    placed = (P(None, "gx", "gy", "agg"), P(None, "gx", "gy", "agg"), P("gx", "gy", "agg"))
    return jax.shard_map(
        functools.partial(on_device, counts),
        mesh=mesh,
        in_specs=placed,
        out_specs=(P(None, "gx", "gy", "agg"), P(None, "gy", ("agg", "gx"), None)),
        check_vma=False,
    )
```

```python
import functools

import jax
import jax.numpy as jnp
import numpy as np
from jax import lax
from jax.experimental import pallas as pl
from jax.experimental.pallas import tpu as pltpu
from jax.sharding import PartitionSpec as P

SWEEPS = 2
COARSE_SWEEPS = 4
LX = 5
MESH = pl.DeviceIdType.MESH

damping = 0.8
keep = 1.0 - damping
root_half = 0.7071067811865476


def local_levels(cells_x):
    return min(LX, cells_x.bit_length() - 1)


def finish_matrix(cells_x, blocks, rows):
    levels = local_levels(cells_x)
    kept = cells_x // 2
    eye = np.eye(blocks * kept).reshape(blocks, kept, blocks * kept)
    width = cells_x >> levels
    approx = eye[:, :width].reshape(blocks * width, -1)
    details, at = [], width
    for level in range(levels, 1, -1):
        width = cells_x >> level
        details.append(eye[:, at : at + width].reshape(blocks * width, -1))
        at += width
    for level in range(levels, LX):
        low, high = approx[0::2], approx[1::2]
        approx, detail = (low + high) * root_half, (low - high) * root_half
        details.insert(0, detail)
    along_x = np.concatenate([approx] + details, axis=0)
    along_y = np.zeros((rows, rows))
    for row in range(0, rows, 2):
        along_y[row, row : row + 2] = root_half
        along_y[row + 1, row : row + 2] = root_half, -root_half
    return np.einsum("qk,yr->yqkr", along_x, along_y).reshape(-1, blocks * kept * rows).astype(np.float32)


def neighbour_sides():
    return [(axis, high) for axis in ("gx", "gy", "agg") for high in (False, True)]


def edge_sides():
    pairs = (("gx", "gy"), ("gx", "agg"), ("gy", "agg"))
    return [((a, p), (b, q)) for a, b in pairs for p in (False, True) for q in (False, True)]


def kernel(
    sizes, v_hbm, f_hbm, r_hbm, m_hbm, vel_ref, comp_ref, v_ref, f_ref, r_ref, m_ref,
    xs_fine, xr_fine, ys_fine, yr_fine, zs_fine, zr_fine,
    xs_coarse, xr_coarse, ys_coarse, yr_coarse, zs_coarse, zr_coarse,
    xs_deep, xr_deep, ys_deep, yr_deep, zs_deep, zr_deep, exy, exz, eyz,
c_send, c_recv, w_buf, send_sem, recv_sem, deep_send_sem, deep_recv_sem, c_send_sem, c_recv_sem, in_sem,
):
    counts = sizes
    C, X, Y, Z = v_ref.shape
    Xc = X // 2
    half = Z // 2
    me = {axis: lax.axis_index(axis) for axis in counts}
    blocks = counts["gx"]
    chunk = Z // blocks

    def exists(axis, high):
        return me[axis] < counts[axis] - 1 if high else me[axis] > 0

    loads = [
        pltpu.make_async_copy(src, dst, in_sem.at[i])
        for i, (src, dst) in enumerate(
            ((v_hbm, v_ref), (f_hbm, f_ref), (r_hbm, r_ref), (m_hbm, m_ref))
        )
    ]
    for load in loads:
        load.start()
    def beside(*sides):
        return {axis: me[axis] + (1 if high else -1) for axis, high in sides}

    barrier = pltpu.get_barrier_semaphore()
    expected = blocks - 1
    for step in range(1, blocks):
        pl.semaphore_signal(
            barrier, inc=1, device_id={"gx": lax.rem(me["gx"] + step, blocks)}, device_id_type=MESH
        )
    for axis, high in neighbour_sides()[2:]:
        there = exists(axis, high)
        expected = expected + there.astype(jnp.int32)

        @pl.when(there)
        def _():
            pl.semaphore_signal(
                barrier, inc=1, device_id={axis: me[axis] + (1 if high else -1)}, device_id_type=MESH
            )

    for (axis_a, high_a), (axis_b, high_b) in edge_sides():
        there = exists(axis_a, high_a) & exists(axis_b, high_b)
        expected = expected + there.astype(jnp.int32)

        @pl.when(there)
        def _():
            pl.semaphore_signal(
                barrier, inc=1, device_id=beside((axis_a, high_a), (axis_b, high_b)), device_id_type=MESH
            )

    received = {
        "gx": (xr_fine, xr_coarse, xr_deep),
        "gy": (yr_fine, yr_coarse, yr_deep),
        "agg": (zr_fine, zr_coarse, zr_deep),
    }
    edges = {("gx", "gy"): exy, ("gx", "agg"): exz, ("gy", "agg"): eyz}
    for (axis_a, high_a), (axis_b, high_b) in edge_sides():
        @pl.when(jnp.logical_not(exists(axis_a, high_a) & exists(axis_b, high_b)))
        def _():
            buffer = edges[axis_a, axis_b]
            for phase in range(buffer.shape[0]):
                buffer[phase, 2 * int(high_a) + int(high_b)] = jnp.zeros(buffer.shape[2:], buffer.dtype)

    for buffer in (ys_coarse, ys_deep):
        buffer[...] = jnp.zeros(buffer.shape, buffer.dtype)
    for axis, high in neighbour_sides():
        @pl.when(jnp.logical_not(exists(axis, high)))
        def _():
            for buffer in received[axis]:
                for phase in range(buffer.shape[0]):
                    buffer[phase, int(high)] = jnp.zeros(buffer.shape[2:], buffer.dtype)

    row = lax.broadcasted_iota(jnp.int32, (Y, Z), 0)
    lane = lax.broadcasted_iota(jnp.int32, (Y, Z), 1)
    zero = jnp.zeros((Y, Z), jnp.float32)

    def pack(fields, width, phase, xs, ys, zs):
        packed = zero
        for c in range(C):
            for x in range(width):
                k = c * width + x
                field = fields[c][x]
                ys[phase, 0, k : k + 1] = field[0:1]
                ys[phase, 1, k : k + 1] = field[Y - 1 : Y]
                packed = jnp.where(lane == k, field[:, 0:1], packed)
                packed = jnp.where(lane == half + k, field[:, Z - 1 : Z], packed)
        zs[phase] = packed

    def copies(fine, phase):
        number = phase if fine else SWEEPS + 1 + phase
        xs, xr, ys, yr, zs, zr = (
            (xs_fine, xr_fine, ys_fine, yr_fine, zs_fine, zr_fine)
            if fine
            else (xs_coarse, xr_coarse, ys_coarse, yr_coarse, zs_coarse, zr_coarse)
        )
        made = []
        for slot, (axis, high) in enumerate(neighbour_sides()):
            side = int(high)
            if axis == "gx":
                if fine and phase == 0:
                    src = v_ref.at[:, X - 1 if high else 0]
                else:
                    src = xs.at[phase, side]
                dst = xr.at[phase, 1 - side]
            elif axis == "gy":
                src, dst = ys.at[phase, side], yr.at[phase, 1 - side]
            else:
                src, dst = zs.at[phase], zr.at[phase, 1 - side]
            made.append((
                axis,
                high,
                pltpu.make_async_remote_copy(
                    src_ref=src,
                    dst_ref=dst,
                    send_sem=send_sem.at[number, slot],
                    recv_sem=recv_sem.at[number, slot],
                    device_id={axis: me[axis] + (1 if high else -1)},
                    device_id_type=MESH,
                ),
            ))
        return made

    def start(fine, phase, axes=("gx", "gy", "agg")):
        for axis, high, copy in copies(fine, phase):
            if axis in axes:
                pl.when(exists(axis, high))(copy.start)

    def send(fine, phase, fields, width):
        xs, ys, zs = fine_send if fine else coarse_send
        for c in range(C):
            xs[phase, 0, c] = fields[c][0]
            xs[phase, 1, c] = fields[c][width - 1]
        start(fine, phase, ("gx",))
        pack(fields, width, phase, xs, ys, zs)
        start(fine, phase, ("gy", "agg"))

    def arrive(fine, phase):
        for axis, high, copy in copies(fine, phase):
            pl.when(exists(axis, not high))(copy.wait_recv)

    def sent(fine, phase):
        for axis, high, copy in copies(fine, phase):
            pl.when(exists(axis, high))(copy.wait_send)

    def inner_sum(fields, width, stride):
        sums = []
        for c in range(C):
            line = []
            for x in range(width):
                field = fields[c][x]
                total = jnp.where(row < stride, zero, pltpu.roll(field, stride, 0))
                total = total + jnp.where(row >= Y - stride, zero, pltpu.roll(field, Y - stride, 0))
                total = total + jnp.where(lane < stride, zero, pltpu.roll(field, stride, 1))
                total = total + jnp.where(lane >= Z - stride, zero, pltpu.roll(field, Z - stride, 1))
                if x > 0:
                    total = total + fields[c][x - 1]
                if x < width - 1:
                    total = total + fields[c][x + 1]
                line.append(total)
            sums.append(line)
        return sums

    def outer_sum(sums, width, stride, faces, repeat=1):
        along_x, along_y, along_z = faces
        result = []
        for c in range(C):
            line = []
            for x in range(width):
                k = c * (width // repeat) + x // repeat
                total = sums[c][x]
                total = total + jnp.where(row < stride, along_y[0][k : k + 1], 0.0)
                total = total + jnp.where(row >= Y - stride, along_y[1][k : k + 1], 0.0)
                total = total + jnp.where(lane < stride, along_z[0][:, k : k + 1], 0.0)
                total = total + jnp.where(lane >= Z - stride, along_z[1][:, k : k + 1], 0.0)
                if x == 0:
                    total = total + along_x[0][c]
                if x == width - 1:
                    total = total + along_x[1][c]
                line.append(total)
            result.append(line)
        return result

    def faces_of(xr, yr, zr, phase):
        return (
            [[xr[phase, side, c] for c in range(C)] for side in range(2)],
            [yr[phase, side] for side in range(2)],
            [pltpu.roll(zr[phase, 0], half, 1), zr[phase, 1]],
        )

    group = Z // 4
    far = {0: 2, 1: 0}

    def deep_copies(phase):
        made = []
        for slot, (first, second) in enumerate(edge_sides()):
            number = 2 * int(first[1]) + int(second[1])
            back = 3 - number
            if second[0] == "gy":
                src, dst = ys_deep.at[phase, int(second[1]), 0], exy.at[phase, back]
            else:
                src, dst = zs_deep.at[phase], (exz if first[0] == "gx" else eyz).at[phase, back]
            made.append(((first, second), src, dst, 6 + slot))
        for slot, (axis, high) in enumerate(neighbour_sides()):
            side = int(high)
            if axis == "gx":
                src, dst = xs_deep.at[phase, side], xr_deep.at[phase, 1 - side]
            elif axis == "gy":
                src, dst = ys_deep.at[phase, side], yr_deep.at[phase, 1 - side]
            else:
                src, dst = zs_deep.at[phase], zr_deep.at[phase, 1 - side]
            made.append((((axis, high),), src, dst, slot))
        return [
            (
                sides,
                pltpu.make_async_remote_copy(
                    src_ref=src,
                    dst_ref=dst,
                    send_sem=deep_send_sem.at[phase, slot],
                    recv_sem=deep_recv_sem.at[phase, slot],
                    device_id=beside(*sides),
                    device_id_type=MESH,
                ),
            )
            for sides, src, dst, slot in made
        ]

    def all_exist(sides, flip):
        there = None
        for axis, high in sides:
            one = exists(axis, high != flip)
            there = one if there is None else there & one
        return there

    def deep_send(phase, fields, width, stride):
        for c in range(C):
            for depth in range(2):
                xs_deep[phase, 0, depth, c] = fields[c][depth]
                xs_deep[phase, 1, depth, c] = fields[c][width - 1 - depth]
        ready = deep_copies(phase)
        for sides, copy in ready:
            if len(sides) == 1 and sides[0][0] == "gx":
                pl.when(all_exist(sides, False))(copy.start)
        packed = zero
        for c in range(C):
            for x in range(width):
                k = c * width + x
                field = fields[c][x]
                for depth in range(2):
                    at = depth * stride
                    ys_deep[phase, 0, depth, k : k + 1] = field[at : at + 1]
                    ys_deep[phase, 1, depth, k : k + 1] = field[Y - 1 - at : Y - at]
                    packed = jnp.where(lane == depth * group + k, field[:, at : at + 1], packed)
                    packed = jnp.where(
                        lane == (2 + depth) * group + k, field[:, Z - 1 - at : Z - at], packed
                    )
        zs_deep[phase] = packed
        for sides, copy in ready:
            if not (len(sides) == 1 and sides[0][0] == "gx"):
                pl.when(all_exist(sides, False))(copy.start)

    def deep_arrive(phase):
        for sides, copy in deep_copies(phase):
            pl.when(all_exist(sides, True))(copy.wait_recv)

    def deep_sent(phase):
        for sides, copy in deep_copies(phase):
            pl.when(all_exist(sides, False))(copy.wait_send)

    def lanes_from(packed, number, shift=0):
        turn = (shift - number * group) % Z
        return pltpu.roll(packed, turn, 1) if turn else packed

    def deep_faces(phase):
        return (
            [[xr_deep[phase, side, 0, c] for c in range(C)] for side in range(2)],
            [yr_deep[phase, side, 0] for side in range(2)],
            [lanes_from(zr_deep[phase, side], far[side]) for side in range(2)],
        )

    def advance_faces(phase, fields, width, stride, faces, added, weight):
        along_x, along_y, along_z = [], [], []
        rows = ys_deep.shape[3]
        k_row = lax.broadcasted_iota(jnp.int32, (rows, Z), 0)
        k_lane = lax.broadcasted_iota(jnp.int32, (rows, Z), 1)
        for side in range(2):
            near = width - 1 if side == 0 else 0
            planes = []
            for c in range(C):
                plane = faces[0][side][c]
                k = c * width + near
                total = xr_deep[phase, side, 1, c] + fields[c][0 if side == 0 else width - 1]
                total = total + jnp.where(
                    row < stride, exy[phase, 2 * side, k : k + 1], pltpu.roll(plane, stride, 0)
                )
                total = total + jnp.where(
                    row >= Y - stride, exy[phase, 2 * side + 1, k : k + 1], pltpu.roll(plane, Y - stride, 0)
                )
                low = exz[phase, 2 * side][:, far[0] * group + k : far[0] * group + k + 1]
                high = exz[phase, 2 * side + 1][:, far[1] * group + k : far[1] * group + k + 1]
                total = total + jnp.where(lane < stride, low, pltpu.roll(plane, stride, 1))
                total = total + jnp.where(lane >= Z - stride, high, pltpu.roll(plane, Z - stride, 1))
                planes.append(keep * plane + added[0][side][c] + weight[0][side][c] * total)
            along_x.append(planes)

            layer = faces[1][side]
            total = yr_deep[phase, side, 1] + ys_deep[phase, side, 0]
            spot = k_row % width
            total = total + jnp.where(
                spot == 0, pltpu.roll(exy[phase, side], rows - (width - 1), 0), pltpu.roll(layer, 1, 0)
            )
            total = total + jnp.where(
                spot == width - 1, pltpu.roll(exy[phase, 2 + side], width - 1, 0), pltpu.roll(layer, rows - 1, 0)
            )
            at = Y - 1 if side == 0 else 0
            ends = []
            for z_side in range(2):
                line = eyz[phase, 2 * side + z_side, at : at + 1]
                chosen = jnp.where(k_lane == far[z_side] * group + k_row, line, 0.0)
                ends.append(jnp.sum(chosen, axis=1, keepdims=True))
            total = total + jnp.where(k_lane < stride, ends[0], pltpu.roll(layer, stride, 1))
            total = total + jnp.where(k_lane >= Z - stride, ends[1], pltpu.roll(layer, Z - stride, 1))
            along_y.append(keep * layer + added[1][side] + weight[1][side] * total)

            layer = faces[2][side]
            total = lanes_from(zr_deep[phase, side], far[side] + 1)
            total = total + lanes_from(zs_deep[phase], 2 - far[side])
            low = lanes_from(eyz[phase, side], far[side])[Y - 1 : Y]
            high = lanes_from(eyz[phase, 2 + side], far[side])[0:1]
            total = total + jnp.where(row < stride, low, pltpu.roll(layer, stride, 0))
            total = total + jnp.where(row >= Y - stride, high, pltpu.roll(layer, Y - stride, 0))
            spot = lane % width
            total = total + jnp.where(
                spot == 0, lanes_from(exz[phase, side], far[side], 1 - width), pltpu.roll(layer, 1, 1)
            )
            total = total + jnp.where(
                spot == width - 1, lanes_from(exz[phase, 2 + side], far[side], width - 1), pltpu.roll(layer, Z - 1, 1)
            )
            along_z.append(keep * layer + added[2][side] + weight[2][side] * total)
        return along_x, along_y, along_z

    fine_recv = (xr_fine, yr_fine, zr_fine)
    coarse_recv = (xr_coarse, yr_coarse, zr_coarse)
    fine_send = (xs_fine, ys_fine, zs_fine)
    coarse_send = (xs_coarse, ys_coarse, zs_coarse)

    loads[0].wait()
    previous = [[v_ref[c, x] for x in range(X)] for c in range(C)]
    pack(previous, X, 0, *fine_send)
    pl.semaphore_wait(barrier, expected)
    start(True, 0)

    kept = X // 2
    levels = local_levels(X)
    even_row = row % 2 == 0
    even_lane = lane % 2 == 0
    combos_per_tile = Z // chunk
    coefficients = []
    for c in range(C):
        approx, details = previous[c], []
        for level in range(levels):
            low, high = approx[0::2], approx[1::2]
            approx = [(a + b) * root_half for a, b in zip(low, high)]
            if level > 0:
                details = [(a - b) * root_half for a, b in zip(low, high)] + details
        line = []
        for field in approx + details:
            swapped = jnp.where(even_lane, pltpu.roll(field, Z - 1, 1), pltpu.roll(field, 1, 1))
            line.append((jnp.where(even_lane, field, -field) + swapped) * root_half)
        coefficients.append(line)
    row8 = lax.broadcasted_iota(jnp.int32, (8, Z), 1)
    parts = Y // 8
    for j in range(blocks):
        for k in range(kept):
            tiles = {}
            for c in range(C):
                for part in range(parts):
                    tile, place = divmod(c * parts + part, combos_per_tile)
                    field = coefficients[c][k][part * 8 : part * 8 + 8]
                    shift = (place * chunk - j * chunk) % Z
                    moved = pltpu.roll(field, shift, 1) if shift else field
                    if tile in tiles:
                        moved = jnp.where((row8 >= place * chunk) & (row8 < (place + 1) * chunk), moved, tiles[tile])
                    tiles[tile] = moved
            for tile, value in tiles.items():
                c_send[j, tile, k] = value

    def c_copy(j, source):
        return pltpu.make_async_remote_copy(
            src_ref=c_send.at[j],
            dst_ref=c_recv.at[source],
            send_sem=c_send_sem.at[j],
            recv_sem=c_recv_sem.at[source],
            device_id={"gx": j},
            device_id_type=MESH,
        )

    for j in range(blocks):
        pl.when(me["gx"] != j)(c_copy(j, me["gx"]).start)

        @pl.when(me["gx"] == j)
        def _():
            c_recv[j] = c_send[j]

    def finish_compressed():
        for j in range(blocks):
            pl.when(me["gx"] != j)(c_copy(j, j).wait_recv)
        loads[3].wait()
        coefs = blocks * kept
        for tile in range(c_send.shape[1]):
            gathered = c_recv[:, tile].reshape(coefs * 8, Z)
            done = lax.dot_general(
                m_ref[...], gathered, (((1,), (0,)), ((), ())),
                precision=lax.Precision.HIGHEST, preferred_element_type=jnp.float32,
            )
            for place in range(combos_per_tile):
                c, part = divmod(tile * combos_per_tile + place, parts)
                if c < C:
                    for y in range(8):
                        comp_ref[c, part * 8 + y] = done[
                            y * coefs : (y + 1) * coefs, place * chunk : (place + 1) * chunk
                        ]

    loads[1].wait()
    loads[2].wait()
    diagonal = [6.0 + r_ref[x] for x in range(X)]
    for x in range(X):
        w_buf[x] = damping / diagonal[x]
    def pooled(planes):
        out = []
        for x in range(0, len(planes), 2):
            total = planes[x] + planes[x + 1]
            total = total + jnp.where(even_row, pltpu.roll(total, Y - 1, 0), pltpu.roll(total, 1, 0))
            total = total + jnp.where(even_lane, pltpu.roll(total, Z - 1, 1), pltpu.roll(total, 1, 1))
            out.append(total * 0.125)
        return out

    coarse_weight = [damping / ((6.0 + 4.0 * mean) * 0.25) for mean in pooled([r_ref[x] for x in range(X)])]
    coarse_step = [0.25 * weight for weight in coarse_weight]
    send(False, 0, [coarse_step] * C, Xc)
    field = previous
    for sweep in range(SWEEPS):
        sums = inner_sum(field, X, 1)
        sums = [[sums[c][x] + f_ref[c, x] for x in range(X)] for c in range(C)]
        arrive(True, sweep)
        sums = outer_sum(sums, X, 1, faces_of(*fine_recv, sweep))
        field = [[keep * field[c][x] + w_buf[x] * sums[c][x] for x in range(X)] for c in range(C)]
        send(True, sweep + 1, field, X)

    sums = inner_sum(field, X, 1)
    sums = [[sums[c][x] + f_ref[c, x] for x in range(X)] for c in range(C)]
    arrive(True, SWEEPS)
    sums = outer_sum(sums, X, 1, faces_of(*fine_recv, SWEEPS))
    coarse_rhs = [
        pooled([sums[c][x] - (6.0 + r_ref[x]) * field[c][x] for x in range(X)]) for c in range(C)
    ]
    correction = [[coarse_weight[x] * coarse_rhs[c][x] for x in range(Xc)] for c in range(C)]
    deep_send(0, correction, Xc, 2)
    finish_compressed()

    def coarse_sweep(current, faces):
        total = outer_sum(inner_sum(current, Xc, 2), Xc, 2, faces)
        return [
            [keep * current[c][x] + first[c][x] + coarse_step[x] * total[c][x] for x in range(Xc)]
            for c in range(C)
        ]

    first = correction
    arrive(False, 0)
    step_faces = faces_of(*coarse_recv, 0)
    deep_arrive(0)
    first_faces = deep_faces(0)
    later_faces = advance_faces(0, correction, Xc, 2, first_faces, first_faces, step_faces)
    correction = coarse_sweep(coarse_sweep(correction, first_faces), later_faces)
    deep_send(1, correction, Xc, 2)
    deep_arrive(1)
    faces = deep_faces(1)
    later_faces = advance_faces(1, correction, Xc, 2, faces, first_faces, step_faces)
    correction = coarse_sweep(correction, faces)
    spread = [[correction[c][x // 2] for x in range(X)] for c in range(C)]
    added = inner_sum(spread, X, 1)
    sums = [[sums[c][x] + added[c][x] for x in range(X)] for c in range(C)]
    sums = outer_sum(sums, X, 1, later_faces, repeat=2)
    for c in range(C):
        for x in range(X):
            vel_ref[c, x] = keep * (field[c][x] + spread[c][x]) + w_buf[x] * sums[c][x]

    for phase in range(SWEEPS + 1):
        sent(True, phase)
    sent(False, 0)
    for phase in range(COARSE_SWEEPS // 2):
        deep_sent(phase)
    for j in range(blocks):
        pl.when(me["gx"] != j)(c_copy(j, me["gx"]).wait_send)


def on_device(counts, velocity_prev, forcing, reaction):
    C, X, Y, Z = velocity_prev.shape
    blocks = counts["gx"]
    kept = X // 2
    chunk = Z // blocks
    tiles = -(-(C * (Y // 8)) // (Z // chunk))
    matrix = jnp.asarray(finish_matrix(X, blocks, 8))
    vmem = pl.BlockSpec(memory_space=pltpu.VMEM)

    def buffers(phases, width):
        return [
            pltpu.VMEM((phases, 2, C, Y, Z), jnp.float32),
            pltpu.VMEM((phases, 2, C, Y, Z), jnp.float32),
            pltpu.VMEM((phases, 2, -(-C * width // 8) * 8, Z), jnp.float32),
            pltpu.VMEM((phases, 2, -(-C * width // 8) * 8, Z), jnp.float32),
            pltpu.VMEM((phases, Y, Z), jnp.float32),
            pltpu.VMEM((phases, 2, Y, Z), jnp.float32),
        ]

    def deep_buffers(phases, width):
        rows = -(-C * width // 8) * 8
        return [
            pltpu.VMEM((phases, 2, 2, C, Y, Z), jnp.float32),
            pltpu.VMEM((phases, 2, 2, C, Y, Z), jnp.float32),
            pltpu.VMEM((phases, 2, 2, rows, Z), jnp.float32),
            pltpu.VMEM((phases, 2, 2, rows, Z), jnp.float32),
            pltpu.VMEM((phases, Y, Z), jnp.float32),
            pltpu.VMEM((phases, 2, Y, Z), jnp.float32),
            pltpu.VMEM((phases, 4, rows, Z), jnp.float32),
            pltpu.VMEM((phases, 4, Y, Z), jnp.float32),
            pltpu.VMEM((phases, 4, Y, Z), jnp.float32),
        ]

    phases = SWEEPS + 2
    velocity, compressed = pl.pallas_call(
        functools.partial(kernel, counts),
        out_shape=(
            jax.ShapeDtypeStruct((C, X, Y, Z), jnp.float32),
            jax.ShapeDtypeStruct((C, Y, kept * blocks, chunk), jnp.float32),
        ),
        in_specs=[pl.BlockSpec(memory_space=pltpu.HBM)] * 4,
        out_specs=(vmem, vmem),
        scratch_shapes=[
            pltpu.VMEM((C, X, Y, Z), jnp.float32),
            pltpu.VMEM((C, X, Y, Z), jnp.float32),
            pltpu.VMEM((X, Y, Z), jnp.float32),
            pltpu.VMEM(matrix.shape, jnp.float32),
        ] + buffers(SWEEPS + 1, X) + buffers(1, X // 2) + deep_buffers(COARSE_SWEEPS // 2, X // 2) + [
            pltpu.VMEM((blocks, tiles, kept, 8, Z), jnp.float32),
            pltpu.VMEM((blocks, tiles, kept, 8, Z), jnp.float32),
            pltpu.VMEM((X, Y, Z), jnp.float32),
            pltpu.SemaphoreType.DMA((phases, 6)),
            pltpu.SemaphoreType.DMA((phases, 6)),
            pltpu.SemaphoreType.DMA((COARSE_SWEEPS // 2, 18)),
            pltpu.SemaphoreType.DMA((COARSE_SWEEPS // 2, 18)),
            pltpu.SemaphoreType.DMA((blocks,)),
            pltpu.SemaphoreType.DMA((blocks,)),
            pltpu.SemaphoreType.DMA((4,)),
        ],
        compiler_params=pltpu.CompilerParams(collective_id=0, has_side_effects=True, vmem_limit_bytes=67043328),
    )(velocity_prev, forcing, reaction, matrix)
    return velocity, jnp.swapaxes(compressed, 2, 3)


def solution(mesh):
    counts = {axis: mesh.shape[axis] for axis in ("agg", "gx", "gy")}
    placed = (P(None, "gx", "gy", "agg"), P(None, "gx", "gy", "agg"), P("gx", "gy", "agg"))
    return jax.shard_map(
        functools.partial(on_device, counts),
        mesh=mesh,
        in_specs=placed,
        out_specs=(P(None, "gx", "gy", "agg"), P(None, "gy", ("agg", "gx"), None)),
        check_vma=False,
    )
```

```python
import functools

import jax
import jax.numpy as jnp
import numpy as np
from jax import lax
from jax.experimental import pallas as pl
from jax.experimental.pallas import tpu as pltpu
from jax.sharding import PartitionSpec as P

SWEEPS = 2
COARSE_SWEEPS = 4
LX = 5
MESH = pl.DeviceIdType.MESH

damping = 0.8
keep = 1.0 - damping
root_half = 0.7071067811865476


def local_levels(cells_x):
    return min(LX, cells_x.bit_length() - 1)


def finish_matrix(cells_x, blocks, rows):
    levels = local_levels(cells_x)
    kept = cells_x // 2
    eye = np.eye(blocks * kept).reshape(blocks, kept, blocks * kept)
    width = cells_x >> levels
    approx = eye[:, :width].reshape(blocks * width, -1)
    details, at = [], width
    for level in range(levels, 1, -1):
        width = cells_x >> level
        details.append(eye[:, at : at + width].reshape(blocks * width, -1))
        at += width
    for level in range(levels, LX):
        low, high = approx[0::2], approx[1::2]
        approx, detail = (low + high) * root_half, (low - high) * root_half
        details.insert(0, detail)
    along_x = np.concatenate([approx] + details, axis=0)
    along_y = np.zeros((rows, rows))
    for row in range(0, rows, 2):
        along_y[row, row : row + 2] = root_half
        along_y[row + 1, row : row + 2] = root_half, -root_half
    return np.einsum("qk,yr->yqkr", along_x, along_y).reshape(-1, blocks * kept * rows).astype(np.float32)


def neighbour_sides():
    return [(axis, high) for axis in ("gx", "gy", "agg") for high in (False, True)]


def edge_sides():
    pairs = (("gx", "gy"), ("gx", "agg"), ("gy", "agg"))
    return [((a, p), (b, q)) for a, b in pairs for p in (False, True) for q in (False, True)]


def kernel(
    sizes, v_hbm, f_hbm, r_hbm, m_hbm, vel_ref, comp_ref, v_ref, f_ref, r_ref, m_ref,
    xs_fine, xr_fine, ys_fine, yr_fine, zs_fine, zr_fine,
    xs_coarse, xr_coarse, ys_coarse, yr_coarse, zs_coarse, zr_coarse,
    xs_deep, xr_deep, ys_deep, yr_deep, zs_deep, zr_deep, exy, exz, eyz,
c_send, c_recv, w_buf, send_sem, recv_sem, deep_send_sem, deep_recv_sem, c_send_sem, c_recv_sem, in_sem,
):
    counts = sizes
    C, X, Y, Z = v_ref.shape
    Xc = X // 2
    half = Z // 2
    me = {axis: lax.axis_index(axis) for axis in counts}
    blocks = counts["gx"]
    chunk = Z // blocks

    def exists(axis, high):
        return me[axis] < counts[axis] - 1 if high else me[axis] > 0

    loads = [
        pltpu.make_async_copy(src, dst, in_sem.at[i])
        for i, (src, dst) in enumerate(
            ((v_hbm, v_ref), (f_hbm, f_ref), (r_hbm, r_ref), (m_hbm, m_ref))
        )
    ]
    for load in loads:
        load.start()
    def beside(*sides):
        return {axis: me[axis] + (1 if high else -1) for axis, high in sides}

    barrier = pltpu.get_barrier_semaphore()
    expected = blocks - 1
    for step in range(1, blocks):
        pl.semaphore_signal(
            barrier, inc=1, device_id={"gx": lax.rem(me["gx"] + step, blocks)}, device_id_type=MESH
        )
    for axis, high in neighbour_sides()[2:]:
        there = exists(axis, high)
        expected = expected + there.astype(jnp.int32)

        @pl.when(there)
        def _():
            pl.semaphore_signal(
                barrier, inc=1, device_id={axis: me[axis] + (1 if high else -1)}, device_id_type=MESH
            )

    for (axis_a, high_a), (axis_b, high_b) in edge_sides():
        there = exists(axis_a, high_a) & exists(axis_b, high_b)
        expected = expected + there.astype(jnp.int32)

        @pl.when(there)
        def _():
            pl.semaphore_signal(
                barrier, inc=1, device_id=beside((axis_a, high_a), (axis_b, high_b)), device_id_type=MESH
            )

    received = {
        "gx": (xr_fine, xr_coarse, xr_deep),
        "gy": (yr_fine, yr_coarse, yr_deep),
        "agg": (zr_fine, zr_coarse, zr_deep),
    }
    edges = {("gx", "gy"): exy, ("gx", "agg"): exz, ("gy", "agg"): eyz}
    for (axis_a, high_a), (axis_b, high_b) in edge_sides():
        @pl.when(jnp.logical_not(exists(axis_a, high_a) & exists(axis_b, high_b)))
        def _():
            buffer = edges[axis_a, axis_b]
            for phase in range(buffer.shape[0]):
                buffer[phase, 2 * int(high_a) + int(high_b)] = jnp.zeros(buffer.shape[2:], buffer.dtype)

    for buffer in (ys_coarse, ys_deep):
        buffer[...] = jnp.zeros(buffer.shape, buffer.dtype)
    for axis, high in neighbour_sides():
        @pl.when(jnp.logical_not(exists(axis, high)))
        def _():
            for buffer in received[axis]:
                for phase in range(buffer.shape[0]):
                    buffer[phase, int(high)] = jnp.zeros(buffer.shape[2:], buffer.dtype)

    row = lax.broadcasted_iota(jnp.int32, (Y, Z), 0)
    lane = lax.broadcasted_iota(jnp.int32, (Y, Z), 1)
    zero = jnp.zeros((Y, Z), jnp.float32)

    def pack(fields, width, phase, xs, ys, zs):
        packed = zero
        for c in range(C):
            for x in range(width):
                k = c * width + x
                field = fields[c][x]
                ys[phase, 0, k : k + 1] = field[0:1]
                ys[phase, 1, k : k + 1] = field[Y - 1 : Y]
                packed = jnp.where(lane == k, field[:, 0:1], packed)
                packed = jnp.where(lane == half + k, field[:, Z - 1 : Z], packed)
        zs[phase] = packed

    def copies(fine, phase):
        number = phase if fine else SWEEPS + 1 + phase
        xs, xr, ys, yr, zs, zr = (
            (xs_fine, xr_fine, ys_fine, yr_fine, zs_fine, zr_fine)
            if fine
            else (xs_coarse, xr_coarse, ys_coarse, yr_coarse, zs_coarse, zr_coarse)
        )
        made = []
        for slot, (axis, high) in enumerate(neighbour_sides()):
            side = int(high)
            if axis == "gx":
                if fine and phase == 0:
                    src = v_ref.at[:, X - 1 if high else 0]
                else:
                    src = xs.at[phase, side]
                dst = xr.at[phase, 1 - side]
            elif axis == "gy":
                src, dst = ys.at[phase, side], yr.at[phase, 1 - side]
            else:
                src, dst = zs.at[phase], zr.at[phase, 1 - side]
            made.append((
                axis,
                high,
                pltpu.make_async_remote_copy(
                    src_ref=src,
                    dst_ref=dst,
                    send_sem=send_sem.at[number, slot],
                    recv_sem=recv_sem.at[number, slot],
                    device_id={axis: me[axis] + (1 if high else -1)},
                    device_id_type=MESH,
                ),
            ))
        return made

    def start(fine, phase, axes=("gx", "gy", "agg")):
        for axis, high, copy in copies(fine, phase):
            if axis in axes:
                pl.when(exists(axis, high))(copy.start)

    def send(fine, phase, fields, width):
        xs, ys, zs = fine_send if fine else coarse_send
        for c in range(C):
            xs[phase, 0, c] = fields[c][0]
            xs[phase, 1, c] = fields[c][width - 1]
        start(fine, phase, ("gx",))
        pack(fields, width, phase, xs, ys, zs)
        start(fine, phase, ("gy", "agg"))

    def arrive(fine, phase):
        for axis, high, copy in copies(fine, phase):
            pl.when(exists(axis, not high))(copy.wait_recv)

    def sent(fine, phase):
        for axis, high, copy in copies(fine, phase):
            pl.when(exists(axis, high))(copy.wait_send)

    def inner_sum(fields, width, stride):
        sums = []
        for c in range(C):
            line = []
            for x in range(width):
                field = fields[c][x]
                total = jnp.where(row < stride, zero, pltpu.roll(field, stride, 0))
                total = total + jnp.where(row >= Y - stride, zero, pltpu.roll(field, Y - stride, 0))
                total = total + jnp.where(lane < stride, zero, pltpu.roll(field, stride, 1))
                total = total + jnp.where(lane >= Z - stride, zero, pltpu.roll(field, Z - stride, 1))
                if x > 0:
                    total = total + fields[c][x - 1]
                if x < width - 1:
                    total = total + fields[c][x + 1]
                line.append(total)
            sums.append(line)
        return sums

    def outer_sum(sums, width, stride, faces, repeat=1):
        along_x, along_y, along_z = faces
        result = []
        for c in range(C):
            line = []
            for x in range(width):
                k = c * (width // repeat) + x // repeat
                total = sums[c][x]
                total = total + jnp.where(row < stride, along_y[0][k : k + 1], 0.0)
                total = total + jnp.where(row >= Y - stride, along_y[1][k : k + 1], 0.0)
                total = total + jnp.where(lane < stride, along_z[0][:, k : k + 1], 0.0)
                total = total + jnp.where(lane >= Z - stride, along_z[1][:, k : k + 1], 0.0)
                if x == 0:
                    total = total + along_x[0][c]
                if x == width - 1:
                    total = total + along_x[1][c]
                line.append(total)
            result.append(line)
        return result

    def faces_of(xr, yr, zr, phase):
        return (
            [[xr[phase, side, c] for c in range(C)] for side in range(2)],
            [yr[phase, side] for side in range(2)],
            [pltpu.roll(zr[phase, 0], half, 1), zr[phase, 1]],
        )

    group = Z // 4
    far = {0: 2, 1: 0}

    def deep_copies(phase):
        made = []
        for slot, (first, second) in enumerate(edge_sides()):
            number = 2 * int(first[1]) + int(second[1])
            back = 3 - number
            if second[0] == "gy":
                src, dst = ys_deep.at[phase, int(second[1]), 0], exy.at[phase, back]
            else:
                src, dst = zs_deep.at[phase], (exz if first[0] == "gx" else eyz).at[phase, back]
            made.append(((first, second), src, dst, 6 + slot))
        for slot, (axis, high) in enumerate(neighbour_sides()):
            side = int(high)
            if axis == "gx":
                src, dst = xs_deep.at[phase, side], xr_deep.at[phase, 1 - side]
            elif axis == "gy":
                src, dst = ys_deep.at[phase, side], yr_deep.at[phase, 1 - side]
            else:
                src, dst = zs_deep.at[phase], zr_deep.at[phase, 1 - side]
            made.append((((axis, high),), src, dst, slot))
        return [
            (
                sides,
                pltpu.make_async_remote_copy(
                    src_ref=src,
                    dst_ref=dst,
                    send_sem=deep_send_sem.at[phase, slot],
                    recv_sem=deep_recv_sem.at[phase, slot],
                    device_id=beside(*sides),
                    device_id_type=MESH,
                ),
            )
            for sides, src, dst, slot in made
        ]

    def all_exist(sides, flip):
        there = None
        for axis, high in sides:
            one = exists(axis, high != flip)
            there = one if there is None else there & one
        return there

    def deep_send(phase, fields, width, stride):
        for c in range(C):
            for depth in range(2):
                xs_deep[phase, 0, depth, c] = fields[c][depth]
                xs_deep[phase, 1, depth, c] = fields[c][width - 1 - depth]
        ready = deep_copies(phase)
        for sides, copy in ready:
            if len(sides) == 1 and sides[0][0] == "gx":
                pl.when(all_exist(sides, False))(copy.start)
        packed = zero
        for c in range(C):
            for x in range(width):
                k = c * width + x
                field = fields[c][x]
                for depth in range(2):
                    at = depth * stride
                    ys_deep[phase, 0, depth, k : k + 1] = field[at : at + 1]
                    ys_deep[phase, 1, depth, k : k + 1] = field[Y - 1 - at : Y - at]
                    packed = jnp.where(lane == depth * group + k, field[:, at : at + 1], packed)
                    packed = jnp.where(
                        lane == (2 + depth) * group + k, field[:, Z - 1 - at : Z - at], packed
                    )
        zs_deep[phase] = packed
        for sides, copy in ready:
            if not (len(sides) == 1 and sides[0][0] == "gx"):
                pl.when(all_exist(sides, False))(copy.start)

    def deep_arrive(phase):
        for sides, copy in deep_copies(phase):
            pl.when(all_exist(sides, True))(copy.wait_recv)

    def deep_sent(phase):
        for sides, copy in deep_copies(phase):
            pl.when(all_exist(sides, False))(copy.wait_send)

    def lanes_from(packed, number, shift=0):
        turn = (shift - number * group) % Z
        return pltpu.roll(packed, turn, 1) if turn else packed

    def deep_faces(phase):
        return (
            [[xr_deep[phase, side, 0, c] for c in range(C)] for side in range(2)],
            [yr_deep[phase, side, 0] for side in range(2)],
            [lanes_from(zr_deep[phase, side], far[side]) for side in range(2)],
        )

    def advance_faces(phase, fields, width, stride, faces, added, weight):
        along_x, along_y, along_z = [], [], []
        rows = ys_deep.shape[3]
        k_row = lax.broadcasted_iota(jnp.int32, (rows, Z), 0)
        k_lane = lax.broadcasted_iota(jnp.int32, (rows, Z), 1)
        for side in range(2):
            near = width - 1 if side == 0 else 0
            planes = []
            for c in range(C):
                plane = faces[0][side][c]
                k = c * width + near
                total = xr_deep[phase, side, 1, c] + fields[c][0 if side == 0 else width - 1]
                total = total + jnp.where(
                    row < stride, exy[phase, 2 * side, k : k + 1], pltpu.roll(plane, stride, 0)
                )
                total = total + jnp.where(
                    row >= Y - stride, exy[phase, 2 * side + 1, k : k + 1], pltpu.roll(plane, Y - stride, 0)
                )
                low = exz[phase, 2 * side][:, far[0] * group + k : far[0] * group + k + 1]
                high = exz[phase, 2 * side + 1][:, far[1] * group + k : far[1] * group + k + 1]
                total = total + jnp.where(lane < stride, low, pltpu.roll(plane, stride, 1))
                total = total + jnp.where(lane >= Z - stride, high, pltpu.roll(plane, Z - stride, 1))
                planes.append(keep * plane + added[0][side][c] + weight[0][side][c] * total)
            along_x.append(planes)

            layer = faces[1][side]
            total = yr_deep[phase, side, 1] + ys_deep[phase, side, 0]
            spot = k_row % width
            total = total + jnp.where(
                spot == 0, pltpu.roll(exy[phase, side], rows - (width - 1), 0), pltpu.roll(layer, 1, 0)
            )
            total = total + jnp.where(
                spot == width - 1, pltpu.roll(exy[phase, 2 + side], width - 1, 0), pltpu.roll(layer, rows - 1, 0)
            )
            at = Y - 1 if side == 0 else 0
            ends = []
            for z_side in range(2):
                line = eyz[phase, 2 * side + z_side, at : at + 1]
                chosen = jnp.where(k_lane == far[z_side] * group + k_row, line, 0.0)
                ends.append(jnp.sum(chosen, axis=1, keepdims=True))
            total = total + jnp.where(k_lane < stride, ends[0], pltpu.roll(layer, stride, 1))
            total = total + jnp.where(k_lane >= Z - stride, ends[1], pltpu.roll(layer, Z - stride, 1))
            along_y.append(keep * layer + added[1][side] + weight[1][side] * total)

            layer = faces[2][side]
            total = lanes_from(zr_deep[phase, side], far[side] + 1)
            total = total + lanes_from(zs_deep[phase], 2 - far[side])
            low = lanes_from(eyz[phase, side], far[side])[Y - 1 : Y]
            high = lanes_from(eyz[phase, 2 + side], far[side])[0:1]
            total = total + jnp.where(row < stride, low, pltpu.roll(layer, stride, 0))
            total = total + jnp.where(row >= Y - stride, high, pltpu.roll(layer, Y - stride, 0))
            spot = lane % width
            total = total + jnp.where(
                spot == 0, lanes_from(exz[phase, side], far[side], 1 - width), pltpu.roll(layer, 1, 1)
            )
            total = total + jnp.where(
                spot == width - 1, lanes_from(exz[phase, 2 + side], far[side], width - 1), pltpu.roll(layer, Z - 1, 1)
            )
            along_z.append(keep * layer + added[2][side] + weight[2][side] * total)
        return along_x, along_y, along_z

    fine_recv = (xr_fine, yr_fine, zr_fine)
    coarse_recv = (xr_coarse, yr_coarse, zr_coarse)
    fine_send = (xs_fine, ys_fine, zs_fine)
    coarse_send = (xs_coarse, ys_coarse, zs_coarse)

    loads[0].wait()
    previous = [[v_ref[c, x] for x in range(X)] for c in range(C)]
    pack(previous, X, 0, *fine_send)
    pl.semaphore_wait(barrier, expected)
    start(True, 0)

    kept = X // 2
    levels = local_levels(X)
    even_row = row % 2 == 0
    even_lane = lane % 2 == 0
    combos_per_tile = Z // chunk
    coefficients = []
    for c in range(C):
        approx, details = previous[c], []
        for level in range(levels):
            low, high = approx[0::2], approx[1::2]
            approx = [(a + b) * root_half for a, b in zip(low, high)]
            if level > 0:
                details = [(a - b) * root_half for a, b in zip(low, high)] + details
        line = []
        for field in approx + details:
            swapped = jnp.where(even_lane, pltpu.roll(field, Z - 1, 1), pltpu.roll(field, 1, 1))
            line.append((jnp.where(even_lane, field, -field) + swapped) * root_half)
        coefficients.append(line)
    row8 = lax.broadcasted_iota(jnp.int32, (8, Z), 1)
    parts = Y // 8
    for j in range(blocks):
        for k in range(kept):
            tiles = {}
            for c in range(C):
                for part in range(parts):
                    tile, place = divmod(c * parts + part, combos_per_tile)
                    field = coefficients[c][k][part * 8 : part * 8 + 8]
                    shift = (place * chunk - j * chunk) % Z
                    moved = pltpu.roll(field, shift, 1) if shift else field
                    if tile in tiles:
                        moved = jnp.where((row8 >= place * chunk) & (row8 < (place + 1) * chunk), moved, tiles[tile])
                    tiles[tile] = moved
            for tile, value in tiles.items():
                c_send[j, tile, k] = value

    def c_copy(j, source):
        return pltpu.make_async_remote_copy(
            src_ref=c_send.at[j],
            dst_ref=c_recv.at[source],
            send_sem=c_send_sem.at[j],
            recv_sem=c_recv_sem.at[source],
            device_id={"gx": j},
            device_id_type=MESH,
        )

    for j in range(blocks):
        pl.when(me["gx"] != j)(c_copy(j, me["gx"]).start)

        @pl.when(me["gx"] == j)
        def _():
            c_recv[j] = c_send[j]

    def finish_compressed():
        for j in range(blocks):
            pl.when(me["gx"] != j)(c_copy(j, j).wait_recv)
        loads[3].wait()
        coefs = blocks * kept
        for tile in range(c_send.shape[1]):
            gathered = c_recv[:, tile].reshape(coefs * 8, Z)
            done = lax.dot_general(
                m_ref[...], gathered, (((1,), (0,)), ((), ())),
                precision=lax.Precision.HIGHEST, preferred_element_type=jnp.float32,
            )
            for place in range(combos_per_tile):
                c, part = divmod(tile * combos_per_tile + place, parts)
                if c < C:
                    for y in range(8):
                        comp_ref[c, part * 8 + y] = done[
                            y * coefs : (y + 1) * coefs, place * chunk : (place + 1) * chunk
                        ]

    loads[1].wait()
    loads[2].wait()
    diagonal = [6.0 + r_ref[x] for x in range(X)]
    for x in range(X):
        w_buf[x] = damping / diagonal[x]
    def pooled(planes):
        out = []
        for x in range(0, len(planes), 2):
            total = planes[x] + planes[x + 1]
            total = total + jnp.where(even_row, pltpu.roll(total, Y - 1, 0), pltpu.roll(total, 1, 0))
            total = total + jnp.where(even_lane, pltpu.roll(total, Z - 1, 1), pltpu.roll(total, 1, 1))
            out.append(total * 0.125)
        return out

    coarse_weight = [damping / ((6.0 + 4.0 * mean) * 0.25) for mean in pooled([r_ref[x] for x in range(X)])]
    coarse_step = [0.25 * weight for weight in coarse_weight]
    send(False, 0, [coarse_step] * C, Xc)
    field = previous
    for sweep in range(SWEEPS):
        sums = inner_sum(field, X, 1)
        sums = [[sums[c][x] + f_ref[c, x] for x in range(X)] for c in range(C)]
        arrive(True, sweep)
        sums = outer_sum(sums, X, 1, faces_of(*fine_recv, sweep))
        field = [[keep * field[c][x] + w_buf[x] * sums[c][x] for x in range(X)] for c in range(C)]
        send(True, sweep + 1, field, X)

    sums = inner_sum(field, X, 1)
    sums = [[sums[c][x] + f_ref[c, x] for x in range(X)] for c in range(C)]
    arrive(True, SWEEPS)
    sums = outer_sum(sums, X, 1, faces_of(*fine_recv, SWEEPS))
    coarse_rhs = [
        pooled([sums[c][x] - (6.0 + r_ref[x]) * field[c][x] for x in range(X)]) for c in range(C)
    ]
    correction = [[coarse_weight[x] * coarse_rhs[c][x] for x in range(Xc)] for c in range(C)]
    deep_send(0, correction, Xc, 2)
    finish_compressed()

    def coarse_sweep(current, faces):
        total = outer_sum(inner_sum(current, Xc, 2), Xc, 2, faces)
        return [
            [keep * current[c][x] + first[c][x] + coarse_step[x] * total[c][x] for x in range(Xc)]
            for c in range(C)
        ]

    first = correction
    arrive(False, 0)
    step_faces = faces_of(*coarse_recv, 0)
    deep_arrive(0)
    first_faces = deep_faces(0)
    later_faces = advance_faces(0, correction, Xc, 2, first_faces, first_faces, step_faces)
    correction = coarse_sweep(coarse_sweep(correction, first_faces), later_faces)
    deep_send(1, correction, Xc, 2)
    deep_arrive(1)
    faces = deep_faces(1)
    later_faces = advance_faces(1, correction, Xc, 2, faces, first_faces, step_faces)
    correction = coarse_sweep(correction, faces)
    spread = [[correction[c][x // 2] for x in range(X)] for c in range(C)]
    added = inner_sum(spread, X, 1)
    sums = [[sums[c][x] + added[c][x] for x in range(X)] for c in range(C)]
    sums = outer_sum(sums, X, 1, later_faces, repeat=2)
    for c in range(C):
        for x in range(X):
            vel_ref[c, x] = keep * (field[c][x] + spread[c][x]) + w_buf[x] * sums[c][x]

    for phase in range(SWEEPS + 1):
        sent(True, phase)
    sent(False, 0)
    for phase in range(COARSE_SWEEPS // 2):
        deep_sent(phase)
    for j in range(blocks):
        pl.when(me["gx"] != j)(c_copy(j, me["gx"]).wait_send)


def on_device(counts, velocity_prev, forcing, reaction):
    C, X, Y, Z = velocity_prev.shape
    blocks = counts["gx"]
    kept = X // 2
    chunk = Z // blocks
    tiles = -(-(C * (Y // 8)) // (Z // chunk))
    matrix = jnp.asarray(finish_matrix(X, blocks, 8))
    vmem = pl.BlockSpec(memory_space=pltpu.VMEM)

    def buffers(phases, width):
        return [
            pltpu.VMEM((phases, 2, C, Y, Z), jnp.float32),
            pltpu.VMEM((phases, 2, C, Y, Z), jnp.float32),
            pltpu.VMEM((phases, 2, -(-C * width // 8) * 8, Z), jnp.float32),
            pltpu.VMEM((phases, 2, -(-C * width // 8) * 8, Z), jnp.float32),
            pltpu.VMEM((phases, Y, Z), jnp.float32),
            pltpu.VMEM((phases, 2, Y, Z), jnp.float32),
        ]

    def deep_buffers(phases, width):
        rows = -(-C * width // 8) * 8
        return [
            pltpu.VMEM((phases, 2, 2, C, Y, Z), jnp.float32),
            pltpu.VMEM((phases, 2, 2, C, Y, Z), jnp.float32),
            pltpu.VMEM((phases, 2, 2, rows, Z), jnp.float32),
            pltpu.VMEM((phases, 2, 2, rows, Z), jnp.float32),
            pltpu.VMEM((phases, Y, Z), jnp.float32),
            pltpu.VMEM((phases, 2, Y, Z), jnp.float32),
            pltpu.VMEM((phases, 4, rows, Z), jnp.float32),
            pltpu.VMEM((phases, 4, Y, Z), jnp.float32),
            pltpu.VMEM((phases, 4, Y, Z), jnp.float32),
        ]

    phases = SWEEPS + 2
    velocity, compressed = pl.pallas_call(
        functools.partial(kernel, counts),
        out_shape=(
            jax.ShapeDtypeStruct((C, X, Y, Z), jnp.float32),
            jax.ShapeDtypeStruct((C, Y, kept * blocks, chunk), jnp.float32),
        ),
        in_specs=[pl.BlockSpec(memory_space=pltpu.HBM)] * 4,
        out_specs=(vmem, vmem),
        scratch_shapes=[
            pltpu.VMEM((C, X, Y, Z), jnp.float32),
            pltpu.VMEM((C, X, Y, Z), jnp.float32),
            pltpu.VMEM((X, Y, Z), jnp.float32),
            pltpu.VMEM(matrix.shape, jnp.float32),
        ] + buffers(SWEEPS + 1, X) + buffers(1, X // 2) + deep_buffers(COARSE_SWEEPS // 2, X // 2) + [
            pltpu.VMEM((blocks, tiles, kept, 8, Z), jnp.float32),
            pltpu.VMEM((blocks, tiles, kept, 8, Z), jnp.float32),
            pltpu.VMEM((X, Y, Z), jnp.float32),
            pltpu.SemaphoreType.DMA((phases, 6)),
            pltpu.SemaphoreType.DMA((phases, 6)),
            pltpu.SemaphoreType.DMA((COARSE_SWEEPS // 2, 18)),
            pltpu.SemaphoreType.DMA((COARSE_SWEEPS // 2, 18)),
            pltpu.SemaphoreType.DMA((blocks,)),
            pltpu.SemaphoreType.DMA((blocks,)),
            pltpu.SemaphoreType.DMA((4,)),
        ],
        compiler_params=pltpu.CompilerParams(collective_id=0, has_side_effects=True, vmem_limit_bytes=40000000),
    )(*(pltpu.with_memory_space_constraint(a, pltpu.HBM) for a in (velocity_prev, forcing, reaction, matrix)))
    return velocity, jnp.swapaxes(compressed, 2, 3)


def solution(mesh):
    counts = {axis: mesh.shape[axis] for axis in ("agg", "gx", "gy")}
    placed = (P(None, "gx", "gy", "agg"), P(None, "gx", "gy", "agg"), P("gx", "gy", "agg"))
    return jax.shard_map(
        functools.partial(on_device, counts),
        mesh=mesh,
        in_specs=placed,
        out_specs=(P(None, "gx", "gy", "agg"), P(None, "gy", ("agg", "gx"), None)),
        check_vma=False,
    )
```

```python
import functools

import jax
import jax.numpy as jnp
import numpy as np
from jax import lax
from jax.experimental import pallas as pl
from jax.experimental.pallas import tpu as pltpu
from jax.sharding import PartitionSpec as P

SWEEPS = 2
COARSE_SWEEPS = 4
LX = 5
MESH = pl.DeviceIdType.MESH

damping = 0.8
keep = 1.0 - damping
root_half = 0.7071067811865476


def local_levels(cells_x):
    return min(LX, cells_x.bit_length() - 1)


def finish_matrix(cells_x, blocks, rows):
    levels = local_levels(cells_x)
    kept = cells_x // 2
    eye = np.eye(blocks * kept).reshape(blocks, kept, blocks * kept)
    width = cells_x >> levels
    approx = eye[:, :width].reshape(blocks * width, -1)
    details, at = [], width
    for level in range(levels, 1, -1):
        width = cells_x >> level
        details.append(eye[:, at : at + width].reshape(blocks * width, -1))
        at += width
    for level in range(levels, LX):
        low, high = approx[0::2], approx[1::2]
        approx, detail = (low + high) * root_half, (low - high) * root_half
        details.insert(0, detail)
    along_x = np.concatenate([approx] + details, axis=0)
    along_y = np.zeros((rows, rows))
    for row in range(0, rows, 2):
        along_y[row, row : row + 2] = root_half
        along_y[row + 1, row : row + 2] = root_half, -root_half
    return np.einsum("qk,yr->yqkr", along_x, along_y).reshape(-1, blocks * kept * rows).astype(np.float32)


def neighbour_sides():
    return [(axis, high) for axis in ("gx", "gy", "agg") for high in (False, True)]


def edge_sides():
    pairs = (("gx", "gy"), ("gx", "agg"), ("gy", "agg"))
    return [((a, p), (b, q)) for a, b in pairs for p in (False, True) for q in (False, True)]


def kernel(
    sizes, v_hbm, f_hbm, r_hbm, m_hbm, vel_ref, comp_ref, v_ref, f_ref, r_ref, m_ref,
    xs_fine, xr_fine, ys_fine, yr_fine, zs_fine, zr_fine,
    xs_coarse, xr_coarse, ys_coarse, yr_coarse, zs_coarse, zr_coarse,
    xs_deep, xr_deep, ys_deep, yr_deep, zs_deep, zr_deep, exy, exz, eyz,
c_send, c_recv, w_buf, send_sem, recv_sem, deep_send_sem, deep_recv_sem, c_send_sem, c_recv_sem, in_sem,
):
    counts = sizes
    C, X, Y, Z = v_ref.shape
    Xc = X // 2
    half = Z // 2
    me = {axis: lax.axis_index(axis) for axis in counts}
    blocks = counts["gx"]
    chunk = Z // blocks

    def exists(axis, high):
        return me[axis] < counts[axis] - 1 if high else me[axis] > 0

    loads = [
        pltpu.make_async_copy(src, dst, in_sem.at[i])
        for i, (src, dst) in enumerate(
            ((v_hbm, v_ref), (f_hbm, f_ref), (r_hbm, r_ref), (m_hbm, m_ref))
        )
    ]
    for load in loads:
        load.start()
    def beside(*sides):
        return {axis: me[axis] + (1 if high else -1) for axis, high in sides}

    barrier = pltpu.get_barrier_semaphore()
    expected = blocks - 1
    for step in range(1, blocks):
        pl.semaphore_signal(
            barrier, inc=1, device_id={"gx": lax.rem(me["gx"] + step, blocks)}, device_id_type=MESH
        )
    for axis, high in neighbour_sides()[2:]:
        there = exists(axis, high)
        expected = expected + there.astype(jnp.int32)

        @pl.when(there)
        def _():
            pl.semaphore_signal(
                barrier, inc=1, device_id={axis: me[axis] + (1 if high else -1)}, device_id_type=MESH
            )

    for (axis_a, high_a), (axis_b, high_b) in edge_sides():
        there = exists(axis_a, high_a) & exists(axis_b, high_b)
        expected = expected + there.astype(jnp.int32)

        @pl.when(there)
        def _():
            pl.semaphore_signal(
                barrier, inc=1, device_id=beside((axis_a, high_a), (axis_b, high_b)), device_id_type=MESH
            )

    received = {
        "gx": (xr_fine, xr_coarse, xr_deep),
        "gy": (yr_fine, yr_coarse, yr_deep),
        "agg": (zr_fine, zr_coarse, zr_deep),
    }
    edges = {("gx", "gy"): exy, ("gx", "agg"): exz, ("gy", "agg"): eyz}
    for (axis_a, high_a), (axis_b, high_b) in edge_sides():
        @pl.when(jnp.logical_not(exists(axis_a, high_a) & exists(axis_b, high_b)))
        def _():
            buffer = edges[axis_a, axis_b]
            for phase in range(buffer.shape[0]):
                buffer[phase, 2 * int(high_a) + int(high_b)] = jnp.zeros(buffer.shape[2:], buffer.dtype)

    for buffer in (ys_coarse, ys_deep):
        buffer[...] = jnp.zeros(buffer.shape, buffer.dtype)
    for axis, high in neighbour_sides():
        @pl.when(jnp.logical_not(exists(axis, high)))
        def _():
            for buffer in received[axis]:
                for phase in range(buffer.shape[0]):
                    buffer[phase, int(high)] = jnp.zeros(buffer.shape[2:], buffer.dtype)

    row = lax.broadcasted_iota(jnp.int32, (Y, Z), 0)
    lane = lax.broadcasted_iota(jnp.int32, (Y, Z), 1)
    zero = jnp.zeros((Y, Z), jnp.float32)

    def pack(fields, width, phase, xs, ys, zs):
        packed = zero
        for c in range(C):
            for x in range(width):
                k = c * width + x
                field = fields[c][x]
                ys[phase, 0, k : k + 1] = field[0:1]
                ys[phase, 1, k : k + 1] = field[Y - 1 : Y]
                packed = jnp.where(lane == k, field[:, 0:1], packed)
                packed = jnp.where(lane == half + k, field[:, Z - 1 : Z], packed)
        zs[phase] = packed

    def copies(fine, phase):
        number = phase if fine else SWEEPS + 1 + phase
        xs, xr, ys, yr, zs, zr = (
            (xs_fine, xr_fine, ys_fine, yr_fine, zs_fine, zr_fine)
            if fine
            else (xs_coarse, xr_coarse, ys_coarse, yr_coarse, zs_coarse, zr_coarse)
        )
        made = []
        for slot, (axis, high) in enumerate(neighbour_sides()):
            side = int(high)
            if axis == "gx":
                if fine and phase == 0:
                    src = v_ref.at[:, X - 1 if high else 0]
                else:
                    src = xs.at[phase, side]
                dst = xr.at[phase, 1 - side]
            elif axis == "gy":
                src, dst = ys.at[phase, side], yr.at[phase, 1 - side]
            else:
                src, dst = zs.at[phase], zr.at[phase, 1 - side]
            made.append((
                axis,
                high,
                pltpu.make_async_remote_copy(
                    src_ref=src,
                    dst_ref=dst,
                    send_sem=send_sem.at[number, slot],
                    recv_sem=recv_sem.at[number, slot],
                    device_id={axis: me[axis] + (1 if high else -1)},
                    device_id_type=MESH,
                ),
            ))
        return made

    def start(fine, phase, axes=("gx", "gy", "agg")):
        for axis, high, copy in copies(fine, phase):
            if axis in axes:
                pl.when(exists(axis, high))(copy.start)

    def send(fine, phase, fields, width):
        xs, ys, zs = fine_send if fine else coarse_send
        for c in range(C):
            xs[phase, 0, c] = fields[c][0]
            xs[phase, 1, c] = fields[c][width - 1]
        start(fine, phase, ("gx",))
        pack(fields, width, phase, xs, ys, zs)
        start(fine, phase, ("gy", "agg"))

    def arrive(fine, phase):
        for axis, high, copy in copies(fine, phase):
            pl.when(exists(axis, not high))(copy.wait_recv)

    def sent(fine, phase):
        for axis, high, copy in copies(fine, phase):
            pl.when(exists(axis, high))(copy.wait_send)

    def inner_sum(fields, width, stride):
        sums = []
        for c in range(C):
            line = []
            for x in range(width):
                field = fields[c][x]
                total = jnp.where(row < stride, zero, pltpu.roll(field, stride, 0))
                total = total + jnp.where(row >= Y - stride, zero, pltpu.roll(field, Y - stride, 0))
                total = total + jnp.where(lane < stride, zero, pltpu.roll(field, stride, 1))
                total = total + jnp.where(lane >= Z - stride, zero, pltpu.roll(field, Z - stride, 1))
                if x > 0:
                    total = total + fields[c][x - 1]
                if x < width - 1:
                    total = total + fields[c][x + 1]
                line.append(total)
            sums.append(line)
        return sums

    def outer_sum(sums, width, stride, faces, repeat=1):
        along_x, along_y, along_z = faces
        result = []
        for c in range(C):
            line = []
            for x in range(width):
                k = c * (width // repeat) + x // repeat
                total = sums[c][x]
                total = total + jnp.where(row < stride, along_y[0][k : k + 1], 0.0)
                total = total + jnp.where(row >= Y - stride, along_y[1][k : k + 1], 0.0)
                total = total + jnp.where(lane < stride, along_z[0][:, k : k + 1], 0.0)
                total = total + jnp.where(lane >= Z - stride, along_z[1][:, k : k + 1], 0.0)
                if x == 0:
                    total = total + along_x[0][c]
                if x == width - 1:
                    total = total + along_x[1][c]
                line.append(total)
            result.append(line)
        return result

    def faces_of(xr, yr, zr, phase):
        return (
            [[xr[phase, side, c] for c in range(C)] for side in range(2)],
            [yr[phase, side] for side in range(2)],
            [pltpu.roll(zr[phase, 0], half, 1), zr[phase, 1]],
        )

    group = Z // 4
    far = {0: 2, 1: 0}

    def rows_of(width):
        return -(-C * width // 8) * 8

    def deep_copies(phase):
        made = []
        rows = pl.ds(0, rows_of(X if phase == 0 else Xc))
        for slot, (first, second) in enumerate(edge_sides()):
            number = 2 * int(first[1]) + int(second[1])
            back = 3 - number
            if second[0] == "gy":
                src, dst = ys_deep.at[phase, int(second[1]), 0, rows], exy.at[phase, back, rows]
            else:
                src, dst = zs_deep.at[phase], (exz if first[0] == "gx" else eyz).at[phase, back]
            made.append(((first, second), src, dst, 6 + slot))
        for slot, (axis, high) in enumerate(neighbour_sides()):
            side = int(high)
            if axis == "gx":
                src, dst = xs_deep.at[phase, side], xr_deep.at[phase, 1 - side]
            elif axis == "gy":
                src, dst = ys_deep.at[phase, side, :, rows], yr_deep.at[phase, 1 - side, :, rows]
            else:
                src, dst = zs_deep.at[phase], zr_deep.at[phase, 1 - side]
            made.append((((axis, high),), src, dst, slot))
        return [
            (
                sides,
                pltpu.make_async_remote_copy(
                    src_ref=src,
                    dst_ref=dst,
                    send_sem=deep_send_sem.at[phase, slot],
                    recv_sem=deep_recv_sem.at[phase, slot],
                    device_id=beside(*sides),
                    device_id_type=MESH,
                ),
            )
            for sides, src, dst, slot in made
        ]

    def all_exist(sides, flip):
        there = None
        for axis, high in sides:
            one = exists(axis, high != flip)
            there = one if there is None else there & one
        return there

    def deep_send(phase, fields, width, stride):
        for c in range(C):
            for depth in range(2):
                xs_deep[phase, 0, depth, c] = fields[c][depth]
                xs_deep[phase, 1, depth, c] = fields[c][width - 1 - depth]
        ready = deep_copies(phase)
        for sides, copy in ready:
            if len(sides) == 1 and sides[0][0] == "gx":
                pl.when(all_exist(sides, False))(copy.start)
        packed = zero
        for c in range(C):
            for x in range(width):
                k = c * width + x
                field = fields[c][x]
                for depth in range(2):
                    at = depth * stride
                    ys_deep[phase, 0, depth, k : k + 1] = field[at : at + 1]
                    ys_deep[phase, 1, depth, k : k + 1] = field[Y - 1 - at : Y - at]
                    packed = jnp.where(lane == depth * group + k, field[:, at : at + 1], packed)
                    packed = jnp.where(
                        lane == (2 + depth) * group + k, field[:, Z - 1 - at : Z - at], packed
                    )
        zs_deep[phase] = packed
        for sides, copy in ready:
            if not (len(sides) == 1 and sides[0][0] == "gx"):
                pl.when(all_exist(sides, False))(copy.start)

    def deep_arrive(phase):
        for sides, copy in deep_copies(phase):
            pl.when(all_exist(sides, True))(copy.wait_recv)

    def deep_sent(phase):
        for sides, copy in deep_copies(phase):
            pl.when(all_exist(sides, False))(copy.wait_send)

    def lanes_from(packed, number, shift=0):
        turn = (shift - number * group) % Z
        return pltpu.roll(packed, turn, 1) if turn else packed

    def deep_faces(phase):
        return (
            [[xr_deep[phase, side, 0, c] for c in range(C)] for side in range(2)],
            [yr_deep[phase, side, 0, : rows_of(X if phase == 0 else Xc)] for side in range(2)],
            [lanes_from(zr_deep[phase, side], far[side]) for side in range(2)],
        )

    def advance_faces(phase, fields, width, stride, faces, added, weight):
        along_x, along_y, along_z = [], [], []
        rows = rows_of(width)
        k_row = lax.broadcasted_iota(jnp.int32, (rows, Z), 0)
        k_lane = lax.broadcasted_iota(jnp.int32, (rows, Z), 1)
        for side in range(2):
            near = width - 1 if side == 0 else 0
            planes = []
            for c in range(C):
                plane = faces[0][side][c]
                k = c * width + near
                total = xr_deep[phase, side, 1, c] + fields[c][0 if side == 0 else width - 1]
                total = total + jnp.where(
                    row < stride, exy[phase, 2 * side, k : k + 1], pltpu.roll(plane, stride, 0)
                )
                total = total + jnp.where(
                    row >= Y - stride, exy[phase, 2 * side + 1, k : k + 1], pltpu.roll(plane, Y - stride, 0)
                )
                low = exz[phase, 2 * side][:, far[0] * group + k : far[0] * group + k + 1]
                high = exz[phase, 2 * side + 1][:, far[1] * group + k : far[1] * group + k + 1]
                total = total + jnp.where(lane < stride, low, pltpu.roll(plane, stride, 1))
                total = total + jnp.where(lane >= Z - stride, high, pltpu.roll(plane, Z - stride, 1))
                planes.append(keep * plane + added[0][side][c] + weight[0][side][c] * total)
            along_x.append(planes)

            layer = faces[1][side]
            total = yr_deep[phase, side, 1, :rows] + ys_deep[phase, side, 0, :rows]
            spot = k_row % width
            total = total + jnp.where(
                spot == 0, pltpu.roll(exy[phase, side, :rows], rows - (width - 1), 0), pltpu.roll(layer, 1, 0)
            )
            total = total + jnp.where(
                spot == width - 1, pltpu.roll(exy[phase, 2 + side, :rows], width - 1, 0), pltpu.roll(layer, rows - 1, 0)
            )
            at = Y - 1 if side == 0 else 0
            ends = []
            for z_side in range(2):
                line = eyz[phase, 2 * side + z_side, at : at + 1]
                chosen = jnp.where(k_lane == far[z_side] * group + k_row, line, 0.0)
                ends.append(jnp.sum(chosen, axis=1, keepdims=True))
            total = total + jnp.where(k_lane < stride, ends[0], pltpu.roll(layer, stride, 1))
            total = total + jnp.where(k_lane >= Z - stride, ends[1], pltpu.roll(layer, Z - stride, 1))
            along_y.append(keep * layer + added[1][side] + weight[1][side] * total)

            layer = faces[2][side]
            total = lanes_from(zr_deep[phase, side], far[side] + 1)
            total = total + lanes_from(zs_deep[phase], 2 - far[side])
            low = lanes_from(eyz[phase, side], far[side])[Y - 1 : Y]
            high = lanes_from(eyz[phase, 2 + side], far[side])[0:1]
            total = total + jnp.where(row < stride, low, pltpu.roll(layer, stride, 0))
            total = total + jnp.where(row >= Y - stride, high, pltpu.roll(layer, Y - stride, 0))
            spot = lane % width
            total = total + jnp.where(
                spot == 0, lanes_from(exz[phase, side], far[side], 1 - width), pltpu.roll(layer, 1, 1)
            )
            total = total + jnp.where(
                spot == width - 1, lanes_from(exz[phase, 2 + side], far[side], width - 1), pltpu.roll(layer, Z - 1, 1)
            )
            along_z.append(keep * layer + added[2][side] + weight[2][side] * total)
        return along_x, along_y, along_z

    fine_recv = (xr_fine, yr_fine, zr_fine)
    coarse_recv = (xr_coarse, yr_coarse, zr_coarse)
    fine_send = (xs_fine, ys_fine, zs_fine)
    coarse_send = (xs_coarse, ys_coarse, zs_coarse)

    loads[0].wait()
    previous = [[v_ref[c, x] for x in range(X)] for c in range(C)]
    pack(previous, X, 0, *fine_send)
    pl.semaphore_wait(barrier, expected)
    start(True, 0)

    loads[1].wait()
    loads[2].wait()
    for x in range(X):
        w_buf[x] = damping / (6.0 + r_ref[x])
    scaled = [[w_buf[x] * f_ref[c, x] for x in range(X)] for c in range(C)]
    send(True, 1, scaled, X)
    send(True, 2, [[w_buf[x] for x in range(X)]] * C, X)

    kept = X // 2
    levels = local_levels(X)
    even_row = row % 2 == 0
    even_lane = lane % 2 == 0
    combos_per_tile = Z // chunk
    coefficients = []
    for c in range(C):
        approx, details = previous[c], []
        for level in range(levels):
            low, high = approx[0::2], approx[1::2]
            approx = [(a + b) * root_half for a, b in zip(low, high)]
            if level > 0:
                details = [(a - b) * root_half for a, b in zip(low, high)] + details
        line = []
        for field in approx + details:
            swapped = jnp.where(even_lane, pltpu.roll(field, Z - 1, 1), pltpu.roll(field, 1, 1))
            line.append((jnp.where(even_lane, field, -field) + swapped) * root_half)
        coefficients.append(line)
    row8 = lax.broadcasted_iota(jnp.int32, (8, Z), 1)
    parts = Y // 8
    for j in range(blocks):
        for k in range(kept):
            tiles = {}
            for c in range(C):
                for part in range(parts):
                    tile, place = divmod(c * parts + part, combos_per_tile)
                    field = coefficients[c][k][part * 8 : part * 8 + 8]
                    shift = (place * chunk - j * chunk) % Z
                    moved = pltpu.roll(field, shift, 1) if shift else field
                    if tile in tiles:
                        moved = jnp.where((row8 >= place * chunk) & (row8 < (place + 1) * chunk), moved, tiles[tile])
                    tiles[tile] = moved
            for tile, value in tiles.items():
                c_send[j, tile, k] = value

    def c_copy(j, source):
        return pltpu.make_async_remote_copy(
            src_ref=c_send.at[j],
            dst_ref=c_recv.at[source],
            send_sem=c_send_sem.at[j],
            recv_sem=c_recv_sem.at[source],
            device_id={"gx": j},
            device_id_type=MESH,
        )

    def finish_compressed():
        for j in range(blocks):
            pl.when(me["gx"] != j)(c_copy(j, j).wait_recv)
        loads[3].wait()
        coefs = blocks * kept
        for tile in range(c_send.shape[1]):
            gathered = c_recv[:, tile].reshape(coefs * 8, Z)
            done = lax.dot_general(
                m_ref[...], gathered, (((1,), (0,)), ((), ())),
                precision=lax.Precision.HIGHEST, preferred_element_type=jnp.float32,
            )
            for place in range(combos_per_tile):
                c, part = divmod(tile * combos_per_tile + place, parts)
                if c < C:
                    for y in range(8):
                        comp_ref[c, part * 8 + y] = done[
                            y * coefs : (y + 1) * coefs, place * chunk : (place + 1) * chunk
                        ]

    def pooled(planes):
        out = []
        for x in range(0, len(planes), 2):
            total = planes[x] + planes[x + 1]
            total = total + jnp.where(even_row, pltpu.roll(total, Y - 1, 0), pltpu.roll(total, 1, 0))
            total = total + jnp.where(even_lane, pltpu.roll(total, Z - 1, 1), pltpu.roll(total, 1, 1))
            out.append(total * 0.125)
        return out

    coarse_weight = [damping / ((6.0 + 4.0 * mean) * 0.25) for mean in pooled([r_ref[x] for x in range(X)])]
    coarse_step = [0.25 * weight for weight in coarse_weight]

    def fine_sums(current):
        inner = inner_sum(current, X, 1)
        return [[inner[c][x] + f_ref[c, x] for x in range(X)] for c in range(C)]

    def fine_sweep(current, total):
        return [[keep * current[c][x] + w_buf[x] * total[c][x] for x in range(X)] for c in range(C)]

    sums = fine_sums(previous)
    arrive(True, 0)
    field = fine_sweep(previous, outer_sum(sums, X, 1, faces_of(*fine_recv, 0)))
    deep_send(0, field, X, 1)
    send(False, 0, [coarse_step] * C, Xc)
    for j in range(blocks):
        pl.when(me["gx"] != j)(c_copy(j, me["gx"]).start)

        @pl.when(me["gx"] == j)
        def _():
            c_recv[j] = c_send[j]

    sums = fine_sums(field)
    arrive(True, 1)
    arrive(True, 2)
    deep_arrive(0)
    faces = deep_faces(0)
    later_faces = advance_faces(
        0, field, X, 1, faces, faces_of(*fine_recv, 1), faces_of(*fine_recv, 2)
    )
    field = fine_sweep(field, outer_sum(sums, X, 1, faces))
    sums = outer_sum(fine_sums(field), X, 1, later_faces)
    coarse_rhs = [
        pooled([sums[c][x] - (6.0 + r_ref[x]) * field[c][x] for x in range(X)]) for c in range(C)
    ]
    correction = [[coarse_weight[x] * coarse_rhs[c][x] for x in range(Xc)] for c in range(C)]
    deep_send(1, correction, Xc, 2)
    finish_compressed()

    def coarse_sweep(current, faces):
        total = outer_sum(inner_sum(current, Xc, 2), Xc, 2, faces)
        return [
            [keep * current[c][x] + first[c][x] + coarse_step[x] * total[c][x] for x in range(Xc)]
            for c in range(C)
        ]

    first = correction
    arrive(False, 0)
    step_faces = faces_of(*coarse_recv, 0)
    deep_arrive(1)
    first_faces = deep_faces(1)
    later_faces = advance_faces(1, correction, Xc, 2, first_faces, first_faces, step_faces)
    correction = coarse_sweep(coarse_sweep(correction, first_faces), later_faces)
    deep_send(2, correction, Xc, 2)
    deep_arrive(2)
    faces = deep_faces(2)
    later_faces = advance_faces(2, correction, Xc, 2, faces, first_faces, step_faces)
    correction = coarse_sweep(correction, faces)
    spread = [[correction[c][x // 2] for x in range(X)] for c in range(C)]
    added = inner_sum(spread, X, 1)
    sums = [[sums[c][x] + added[c][x] for x in range(X)] for c in range(C)]
    sums = outer_sum(sums, X, 1, later_faces, repeat=2)
    for c in range(C):
        for x in range(X):
            vel_ref[c, x] = keep * (field[c][x] + spread[c][x]) + w_buf[x] * sums[c][x]

    for phase in range(SWEEPS + 1):
        sent(True, phase)
    sent(False, 0)
    for phase in range(1 + COARSE_SWEEPS // 2):
        deep_sent(phase)
    for j in range(blocks):
        pl.when(me["gx"] != j)(c_copy(j, me["gx"]).wait_send)


def on_device(counts, velocity_prev, forcing, reaction):
    C, X, Y, Z = velocity_prev.shape
    blocks = counts["gx"]
    kept = X // 2
    chunk = Z // blocks
    tiles = -(-(C * (Y // 8)) // (Z // chunk))
    matrix = jnp.asarray(finish_matrix(X, blocks, 8))
    vmem = pl.BlockSpec(memory_space=pltpu.VMEM)

    def buffers(phases, width):
        return [
            pltpu.VMEM((phases, 2, C, Y, Z), jnp.float32),
            pltpu.VMEM((phases, 2, C, Y, Z), jnp.float32),
            pltpu.VMEM((phases, 2, -(-C * width // 8) * 8, Z), jnp.float32),
            pltpu.VMEM((phases, 2, -(-C * width // 8) * 8, Z), jnp.float32),
            pltpu.VMEM((phases, Y, Z), jnp.float32),
            pltpu.VMEM((phases, 2, Y, Z), jnp.float32),
        ]

    def deep_buffers(phases, width):
        rows = -(-C * width // 8) * 8
        return [
            pltpu.VMEM((phases, 2, 2, C, Y, Z), jnp.float32),
            pltpu.VMEM((phases, 2, 2, C, Y, Z), jnp.float32),
            pltpu.VMEM((phases, 2, 2, rows, Z), jnp.float32),
            pltpu.VMEM((phases, 2, 2, rows, Z), jnp.float32),
            pltpu.VMEM((phases, Y, Z), jnp.float32),
            pltpu.VMEM((phases, 2, Y, Z), jnp.float32),
            pltpu.VMEM((phases, 4, rows, Z), jnp.float32),
            pltpu.VMEM((phases, 4, Y, Z), jnp.float32),
            pltpu.VMEM((phases, 4, Y, Z), jnp.float32),
        ]

    phases = SWEEPS + 2
    velocity, compressed = pl.pallas_call(
        functools.partial(kernel, counts),
        out_shape=(
            jax.ShapeDtypeStruct((C, X, Y, Z), jnp.float32),
            jax.ShapeDtypeStruct((C, Y, kept * blocks, chunk), jnp.float32),
        ),
        in_specs=[pl.BlockSpec(memory_space=pltpu.HBM)] * 4,
        out_specs=(vmem, vmem),
        scratch_shapes=[
            pltpu.VMEM((C, X, Y, Z), jnp.float32),
            pltpu.VMEM((C, X, Y, Z), jnp.float32),
            pltpu.VMEM((X, Y, Z), jnp.float32),
            pltpu.VMEM(matrix.shape, jnp.float32),
        ] + buffers(SWEEPS + 1, X) + buffers(1, X // 2) + deep_buffers(1 + COARSE_SWEEPS // 2, X) + [
            pltpu.VMEM((blocks, tiles, kept, 8, Z), jnp.float32),
            pltpu.VMEM((blocks, tiles, kept, 8, Z), jnp.float32),
            pltpu.VMEM((X, Y, Z), jnp.float32),
            pltpu.SemaphoreType.DMA((phases, 6)),
            pltpu.SemaphoreType.DMA((phases, 6)),
            pltpu.SemaphoreType.DMA((1 + COARSE_SWEEPS // 2, 18)),
            pltpu.SemaphoreType.DMA((1 + COARSE_SWEEPS // 2, 18)),
            pltpu.SemaphoreType.DMA((blocks,)),
            pltpu.SemaphoreType.DMA((blocks,)),
            pltpu.SemaphoreType.DMA((4,)),
        ],
        compiler_params=pltpu.CompilerParams(collective_id=0, has_side_effects=True, vmem_limit_bytes=40000000),
    )(*(pltpu.with_memory_space_constraint(a, pltpu.HBM) for a in (velocity_prev, forcing, reaction, matrix)))
    return velocity, jnp.swapaxes(compressed, 2, 3)


def solution(mesh):
    counts = {axis: mesh.shape[axis] for axis in ("agg", "gx", "gy")}
    placed = (P(None, "gx", "gy", "agg"), P(None, "gx", "gy", "agg"), P("gx", "gy", "agg"))
    return jax.shard_map(
        functools.partial(on_device, counts),
        mesh=mesh,
        in_specs=placed,
        out_specs=(P(None, "gx", "gy", "agg"), P(None, "gy", ("agg", "gx"), None)),
        check_vma=False,
    )
```

```python
import functools

import jax
import jax.numpy as jnp
import numpy as np
from jax import lax
from jax.experimental import pallas as pl
from jax.experimental.pallas import tpu as pltpu
from jax.sharding import PartitionSpec as P

SWEEPS = 2
COARSE_SWEEPS = 4
LX = 5
MESH = pl.DeviceIdType.MESH

damping = 0.8
keep = 1.0 - damping
root_half = 0.7071067811865476


def local_levels(cells_x):
    return min(LX, cells_x.bit_length() - 1)


def finish_matrix(cells_x, blocks, rows):
    levels = local_levels(cells_x)
    kept = cells_x // 2
    eye = np.eye(blocks * kept).reshape(blocks, kept, blocks * kept)
    width = cells_x >> levels
    approx = eye[:, :width].reshape(blocks * width, -1)
    details, at = [], width
    for level in range(levels, 1, -1):
        width = cells_x >> level
        details.append(eye[:, at : at + width].reshape(blocks * width, -1))
        at += width
    for level in range(levels, LX):
        low, high = approx[0::2], approx[1::2]
        approx, detail = (low + high) * root_half, (low - high) * root_half
        details.insert(0, detail)
    along_x = np.concatenate([approx] + details, axis=0)
    along_y = np.zeros((rows, rows))
    for row in range(0, rows, 2):
        along_y[row, row : row + 2] = root_half
        along_y[row + 1, row : row + 2] = root_half, -root_half
    return np.einsum("qk,yr->yqkr", along_x, along_y).reshape(-1, blocks * kept * rows).astype(np.float32)


def neighbour_sides():
    return [(axis, high) for axis in ("gx", "gy", "agg") for high in (False, True)]


def edge_sides():
    pairs = (("gx", "gy"), ("gx", "agg"), ("gy", "agg"))
    return [((a, p), (b, q)) for a, b in pairs for p in (False, True) for q in (False, True)]


def kernel(
    sizes, v_hbm, f_hbm, r_hbm, m_hbm, vel_ref, comp_ref, v_ref, f_ref, r_ref, m_ref,
    xs_fine, xr_fine, ys_fine, yr_fine, zs_fine, zr_fine,
    xs_coarse, xr_coarse, ys_coarse, yr_coarse, zs_coarse, zr_coarse,
    xs_deep, xr_deep, ys_deep, yr_deep, zs_deep, zr_deep, exy, exz, eyz,
c_send, c_recv, w_buf, send_sem, recv_sem, deep_send_sem, deep_recv_sem, c_send_sem, c_recv_sem, in_sem,
):
    counts = sizes
    C, X, Y, Z = v_ref.shape
    Xc = X // 2
    half = Z // 2
    me = {axis: lax.axis_index(axis) for axis in counts}
    blocks = counts["gx"]
    chunk = Z // blocks

    def exists(axis, high):
        return me[axis] < counts[axis] - 1 if high else me[axis] > 0

    loads = [
        pltpu.make_async_copy(src, dst, in_sem.at[i])
        for i, (src, dst) in enumerate(
            ((v_hbm, v_ref), (f_hbm, f_ref), (r_hbm, r_ref), (m_hbm, m_ref))
        )
    ]
    for load in loads:
        load.start()
    def beside(*sides):
        return {axis: me[axis] + (1 if high else -1) for axis, high in sides}

    barrier = pltpu.get_barrier_semaphore()
    expected = blocks - 1
    for step in range(1, blocks):
        pl.semaphore_signal(
            barrier, inc=1, device_id={"gx": lax.rem(me["gx"] + step, blocks)}, device_id_type=MESH
        )
    for axis, high in neighbour_sides()[2:]:
        there = exists(axis, high)
        expected = expected + there.astype(jnp.int32)

        @pl.when(there)
        def _():
            pl.semaphore_signal(
                barrier, inc=1, device_id={axis: me[axis] + (1 if high else -1)}, device_id_type=MESH
            )

    for (axis_a, high_a), (axis_b, high_b) in edge_sides():
        there = exists(axis_a, high_a) & exists(axis_b, high_b)
        expected = expected + there.astype(jnp.int32)

        @pl.when(there)
        def _():
            pl.semaphore_signal(
                barrier, inc=1, device_id=beside((axis_a, high_a), (axis_b, high_b)), device_id_type=MESH
            )

    received = {
        "gx": (xr_fine, xr_coarse, xr_deep),
        "gy": (yr_fine, yr_coarse, yr_deep),
        "agg": (zr_fine, zr_coarse, zr_deep),
    }
    edges = {("gx", "gy"): exy, ("gx", "agg"): exz, ("gy", "agg"): eyz}
    for (axis_a, high_a), (axis_b, high_b) in edge_sides():
        @pl.when(jnp.logical_not(exists(axis_a, high_a) & exists(axis_b, high_b)))
        def _():
            buffer = edges[axis_a, axis_b]
            for phase in range(buffer.shape[0]):
                buffer[phase, 2 * int(high_a) + int(high_b)] = jnp.zeros(buffer.shape[2:], buffer.dtype)

    for buffer in (ys_coarse, ys_deep):
        buffer[...] = jnp.zeros(buffer.shape, buffer.dtype)
    for axis, high in neighbour_sides():
        @pl.when(jnp.logical_not(exists(axis, high)))
        def _():
            for buffer in received[axis]:
                for phase in range(buffer.shape[0]):
                    buffer[phase, int(high)] = jnp.zeros(buffer.shape[2:], buffer.dtype)

    row = lax.broadcasted_iota(jnp.int32, (Y, Z), 0)
    lane = lax.broadcasted_iota(jnp.int32, (Y, Z), 1)
    zero = jnp.zeros((Y, Z), jnp.float32)

    def pack(fields, width, phase, xs, ys, zs):
        packed = zero
        for c in range(C):
            for x in range(width):
                k = c * width + x
                field = fields[c][x]
                ys[phase, 0, k : k + 1] = field[0:1]
                ys[phase, 1, k : k + 1] = field[Y - 1 : Y]
                packed = jnp.where(lane == k, field[:, 0:1], packed)
                packed = jnp.where(lane == half + k, field[:, Z - 1 : Z], packed)
        zs[phase] = packed

    def copies(fine, phase):
        number = phase if fine else SWEEPS + 1 + phase
        xs, xr, ys, yr, zs, zr = (
            (xs_fine, xr_fine, ys_fine, yr_fine, zs_fine, zr_fine)
            if fine
            else (xs_coarse, xr_coarse, ys_coarse, yr_coarse, zs_coarse, zr_coarse)
        )
        made = []
        for slot, (axis, high) in enumerate(neighbour_sides()):
            side = int(high)
            if axis == "gx":
                if fine and phase == 0:
                    src = v_ref.at[:, X - 1 if high else 0]
                else:
                    src = xs.at[phase, side]
                dst = xr.at[phase, 1 - side]
            elif axis == "gy":
                src, dst = ys.at[phase, side], yr.at[phase, 1 - side]
            else:
                src, dst = zs.at[phase], zr.at[phase, 1 - side]
            made.append((
                axis,
                high,
                pltpu.make_async_remote_copy(
                    src_ref=src,
                    dst_ref=dst,
                    send_sem=send_sem.at[number, slot],
                    recv_sem=recv_sem.at[number, slot],
                    device_id={axis: me[axis] + (1 if high else -1)},
                    device_id_type=MESH,
                ),
            ))
        return made

    def start(fine, phase, axes=("gx", "gy", "agg")):
        for axis, high, copy in copies(fine, phase):
            if axis in axes:
                pl.when(exists(axis, high))(copy.start)

    def send(fine, phase, fields, width):
        xs, ys, zs = fine_send if fine else coarse_send
        for c in range(C):
            xs[phase, 0, c] = fields[c][0]
            xs[phase, 1, c] = fields[c][width - 1]
        start(fine, phase, ("gx",))
        pack(fields, width, phase, xs, ys, zs)
        start(fine, phase, ("gy", "agg"))

    def arrive(fine, phase):
        for axis, high, copy in copies(fine, phase):
            pl.when(exists(axis, not high))(copy.wait_recv)

    def sent(fine, phase):
        for axis, high, copy in copies(fine, phase):
            pl.when(exists(axis, high))(copy.wait_send)

    def inner_sum(fields, width, stride):
        sums = []
        for c in range(C):
            line = []
            for x in range(width):
                field = fields[c][x]
                total = jnp.where(row < stride, zero, pltpu.roll(field, stride, 0))
                total = total + jnp.where(row >= Y - stride, zero, pltpu.roll(field, Y - stride, 0))
                total = total + jnp.where(lane < stride, zero, pltpu.roll(field, stride, 1))
                total = total + jnp.where(lane >= Z - stride, zero, pltpu.roll(field, Z - stride, 1))
                if x > 0:
                    total = total + fields[c][x - 1]
                if x < width - 1:
                    total = total + fields[c][x + 1]
                line.append(total)
            sums.append(line)
        return sums

    def outer_sum(sums, width, stride, faces, repeat=1):
        along_x, along_y, along_z = faces
        result = []
        for c in range(C):
            line = []
            for x in range(width):
                k = c * (width // repeat) + x // repeat
                total = sums[c][x]
                total = total + jnp.where(row < stride, along_y[0][k : k + 1], 0.0)
                total = total + jnp.where(row >= Y - stride, along_y[1][k : k + 1], 0.0)
                total = total + jnp.where(lane < stride, along_z[0][:, k : k + 1], 0.0)
                total = total + jnp.where(lane >= Z - stride, along_z[1][:, k : k + 1], 0.0)
                if x == 0:
                    total = total + along_x[0][c]
                if x == width - 1:
                    total = total + along_x[1][c]
                line.append(total)
            result.append(line)
        return result

    def faces_of(xr, yr, zr, phase):
        return (
            [[xr[phase, side, c] for c in range(C)] for side in range(2)],
            [yr[phase, side] for side in range(2)],
            [pltpu.roll(zr[phase, 0], half, 1), zr[phase, 1]],
        )

    group = Z // 4
    far = {0: 2, 1: 0}

    def rows_of(width):
        return -(-C * width // 8) * 8

    def deep_copies(phase):
        made = []
        rows = pl.ds(0, rows_of(X if phase == 0 else Xc))
        for slot, (first, second) in enumerate(edge_sides()):
            number = 2 * int(first[1]) + int(second[1])
            back = 3 - number
            if second[0] == "gy":
                src, dst = ys_deep.at[phase, int(second[1]), 0, rows], exy.at[phase, back, rows]
            else:
                src, dst = zs_deep.at[phase], (exz if first[0] == "gx" else eyz).at[phase, back]
            made.append(((first, second), src, dst, 6 + slot))
        for slot, (axis, high) in enumerate(neighbour_sides()):
            side = int(high)
            if axis == "gx":
                src, dst = xs_deep.at[phase, side], xr_deep.at[phase, 1 - side]
            elif axis == "gy":
                src, dst = ys_deep.at[phase, side, :, rows], yr_deep.at[phase, 1 - side, :, rows]
            else:
                src, dst = zs_deep.at[phase], zr_deep.at[phase, 1 - side]
            made.append((((axis, high),), src, dst, slot))
        return [
            (
                sides,
                pltpu.make_async_remote_copy(
                    src_ref=src,
                    dst_ref=dst,
                    send_sem=deep_send_sem.at[phase, slot],
                    recv_sem=deep_recv_sem.at[phase, slot],
                    device_id=beside(*sides),
                    device_id_type=MESH,
                ),
            )
            for sides, src, dst, slot in made
        ]

    def all_exist(sides, flip):
        there = None
        for axis, high in sides:
            one = exists(axis, high != flip)
            there = one if there is None else there & one
        return there

    def deep_send(phase, fields, width, stride):
        for c in range(C):
            for depth in range(2):
                xs_deep[phase, 0, depth, c] = fields[c][depth]
                xs_deep[phase, 1, depth, c] = fields[c][width - 1 - depth]
        ready = deep_copies(phase)
        for sides, copy in ready:
            if len(sides) == 1 and sides[0][0] == "gx":
                pl.when(all_exist(sides, False))(copy.start)
        packed = zero
        for c in range(C):
            for x in range(width):
                k = c * width + x
                field = fields[c][x]
                for depth in range(2):
                    at = depth * stride
                    ys_deep[phase, 0, depth, k : k + 1] = field[at : at + 1]
                    ys_deep[phase, 1, depth, k : k + 1] = field[Y - 1 - at : Y - at]
                    packed = jnp.where(lane == depth * group + k, field[:, at : at + 1], packed)
                    packed = jnp.where(
                        lane == (2 + depth) * group + k, field[:, Z - 1 - at : Z - at], packed
                    )
        zs_deep[phase] = packed
        for sides, copy in ready:
            if not (len(sides) == 1 and sides[0][0] == "gx"):
                pl.when(all_exist(sides, False))(copy.start)

    def deep_arrive(phase):
        for sides, copy in deep_copies(phase):
            pl.when(all_exist(sides, True))(copy.wait_recv)

    def deep_sent(phase):
        for sides, copy in deep_copies(phase):
            pl.when(all_exist(sides, False))(copy.wait_send)

    def lanes_from(packed, number, shift=0):
        turn = (shift - number * group) % Z
        return pltpu.roll(packed, turn, 1) if turn else packed

    def deep_faces(phase):
        return (
            [[xr_deep[phase, side, 0, c] for c in range(C)] for side in range(2)],
            [yr_deep[phase, side, 0, : rows_of(X if phase == 0 else Xc)] for side in range(2)],
            [lanes_from(zr_deep[phase, side], far[side]) for side in range(2)],
        )

    def advance_faces(phase, fields, width, stride, faces, added, weight):
        along_x, along_y, along_z = [], [], []
        rows = rows_of(width)
        k_row = lax.broadcasted_iota(jnp.int32, (rows, Z), 0)
        k_lane = lax.broadcasted_iota(jnp.int32, (rows, Z), 1)
        for side in range(2):
            near = width - 1 if side == 0 else 0
            planes = []
            for c in range(C):
                plane = faces[0][side][c]
                k = c * width + near
                total = xr_deep[phase, side, 1, c] + fields[c][0 if side == 0 else width - 1]
                total = total + jnp.where(
                    row < stride, exy[phase, 2 * side, k : k + 1], pltpu.roll(plane, stride, 0)
                )
                total = total + jnp.where(
                    row >= Y - stride, exy[phase, 2 * side + 1, k : k + 1], pltpu.roll(plane, Y - stride, 0)
                )
                low = exz[phase, 2 * side][:, far[0] * group + k : far[0] * group + k + 1]
                high = exz[phase, 2 * side + 1][:, far[1] * group + k : far[1] * group + k + 1]
                total = total + jnp.where(lane < stride, low, pltpu.roll(plane, stride, 1))
                total = total + jnp.where(lane >= Z - stride, high, pltpu.roll(plane, Z - stride, 1))
                planes.append(keep * plane + added[0][side][c] + weight[0][side][c] * total)
            along_x.append(planes)

            layer = faces[1][side]
            total = yr_deep[phase, side, 1, :rows] + ys_deep[phase, side, 0, :rows]
            spot = k_row % width
            total = total + jnp.where(
                spot == 0, pltpu.roll(exy[phase, side, :rows], rows - (width - 1), 0), pltpu.roll(layer, 1, 0)
            )
            total = total + jnp.where(
                spot == width - 1, pltpu.roll(exy[phase, 2 + side, :rows], width - 1, 0), pltpu.roll(layer, rows - 1, 0)
            )
            at = Y - 1 if side == 0 else 0
            ends = []
            for z_side in range(2):
                line = eyz[phase, 2 * side + z_side, at : at + 1]
                chosen = jnp.where(k_lane == far[z_side] * group + k_row, line, 0.0)
                ends.append(jnp.sum(chosen, axis=1, keepdims=True))
            total = total + jnp.where(k_lane < stride, ends[0], pltpu.roll(layer, stride, 1))
            total = total + jnp.where(k_lane >= Z - stride, ends[1], pltpu.roll(layer, Z - stride, 1))
            along_y.append(keep * layer + added[1][side] + weight[1][side] * total)

            layer = faces[2][side]
            total = lanes_from(zr_deep[phase, side], far[side] + 1)
            total = total + lanes_from(zs_deep[phase], 2 - far[side])
            low = lanes_from(eyz[phase, side], far[side])[Y - 1 : Y]
            high = lanes_from(eyz[phase, 2 + side], far[side])[0:1]
            total = total + jnp.where(row < stride, low, pltpu.roll(layer, stride, 0))
            total = total + jnp.where(row >= Y - stride, high, pltpu.roll(layer, Y - stride, 0))
            spot = lane % width
            total = total + jnp.where(
                spot == 0, lanes_from(exz[phase, side], far[side], 1 - width), pltpu.roll(layer, 1, 1)
            )
            total = total + jnp.where(
                spot == width - 1, lanes_from(exz[phase, 2 + side], far[side], width - 1), pltpu.roll(layer, Z - 1, 1)
            )
            along_z.append(keep * layer + added[2][side] + weight[2][side] * total)
        return along_x, along_y, along_z

    fine_recv = (xr_fine, yr_fine, zr_fine)
    coarse_recv = (xr_coarse, yr_coarse, zr_coarse)
    fine_send = (xs_fine, ys_fine, zs_fine)
    coarse_send = (xs_coarse, ys_coarse, zs_coarse)

    loads[0].wait()
    previous = [[v_ref[c, x] for x in range(X)] for c in range(C)]
    pack(previous, X, 0, *fine_send)
    pl.semaphore_wait(barrier, expected)
    start(True, 0)

    loads[1].wait()
    loads[2].wait()
    for x in range(X):
        w_buf[x] = damping / (6.0 + r_ref[x])
    scaled = [[w_buf[x] * f_ref[c, x] for x in range(X)] for c in range(C)]
    send(True, 1, scaled, X)
    send(True, 2, [[w_buf[x] for x in range(X)]] * C, X)

    kept = X // 2
    parts = Y // 8
    even_row = row % 2 == 0
    even_lane = lane % 2 == 0
    combos_per_tile = Z // chunk
    def c_copy(j, source):
        return pltpu.make_async_remote_copy(
            src_ref=c_send.at[j],
            dst_ref=c_recv.at[source],
            send_sem=c_send_sem.at[j],
            recv_sem=c_recv_sem.at[source],
            device_id={"gx": j},
            device_id_type=MESH,
        )

    def finish_compressed(tiles):
        coefs = blocks * kept
        for tile in tiles:
            gathered = c_recv[:, tile].reshape(coefs * 8, Z)
            done = lax.dot_general(
                m_ref[...], gathered, (((1,), (0,)), ((), ())),
                precision=lax.Precision.HIGHEST, preferred_element_type=jnp.float32,
            )
            for place in range(combos_per_tile):
                c, part = divmod(tile * combos_per_tile + place, parts)
                if c < C:
                    for y in range(8):
                        comp_ref[c, part * 8 + y] = done[
                            y * coefs : (y + 1) * coefs, place * chunk : (place + 1) * chunk
                        ]

    def pooled(planes):
        out = []
        for x in range(0, len(planes), 2):
            total = planes[x] + planes[x + 1]
            total = total + jnp.where(even_row, pltpu.roll(total, Y - 1, 0), pltpu.roll(total, 1, 0))
            total = total + jnp.where(even_lane, pltpu.roll(total, Z - 1, 1), pltpu.roll(total, 1, 1))
            out.append(total * 0.125)
        return out

    coarse_weight = [damping / ((6.0 + 4.0 * mean) * 0.25) for mean in pooled([r_ref[x] for x in range(X)])]
    coarse_step = [0.25 * weight for weight in coarse_weight]

    def fine_sums(current):
        inner = inner_sum(current, X, 1)
        return [[inner[c][x] + f_ref[c, x] for x in range(X)] for c in range(C)]

    def fine_sweep(current, total):
        return [[keep * current[c][x] + w_buf[x] * total[c][x] for x in range(X)] for c in range(C)]

    sums = fine_sums(previous)
    arrive(True, 0)
    field = fine_sweep(previous, outer_sum(sums, X, 1, faces_of(*fine_recv, 0)))
    deep_send(0, field, X, 1)
    send(False, 0, [coarse_step] * C, Xc)

    levels = local_levels(X)
    coefficients = []
    for c in range(C):
        approx, details = previous[c], []
        for level in range(levels):
            low, high = approx[0::2], approx[1::2]
            approx = [(a + b) * root_half for a, b in zip(low, high)]
            if level > 0:
                details = [(a - b) * root_half for a, b in zip(low, high)] + details
        line = []
        for values in approx + details:
            swapped = jnp.where(even_lane, pltpu.roll(values, Z - 1, 1), pltpu.roll(values, 1, 1))
            line.append((jnp.where(even_lane, values, -values) + swapped) * root_half)
        coefficients.append(line)
    row8 = lax.broadcasted_iota(jnp.int32, (8, Z), 1)
    for j in range(blocks):
        for k in range(kept):
            tiles = {}
            for c in range(C):
                for part in range(parts):
                    tile, place = divmod(c * parts + part, combos_per_tile)
                    values = coefficients[c][k][part * 8 : part * 8 + 8]
                    shift = (place * chunk - j * chunk) % Z
                    moved = pltpu.roll(values, shift, 1) if shift else values
                    if tile in tiles:
                        moved = jnp.where((row8 >= place * chunk) & (row8 < (place + 1) * chunk), moved, tiles[tile])
                    tiles[tile] = moved
            for tile, value in tiles.items():
                c_send[j, tile, k] = value

    for j in range(blocks):
        pl.when(me["gx"] != j)(c_copy(j, me["gx"]).start)

        @pl.when(me["gx"] == j)
        def _():
            c_recv[j] = c_send[j]

    sums = fine_sums(field)
    arrive(True, 1)
    arrive(True, 2)
    deep_arrive(0)
    faces = deep_faces(0)
    later_faces = advance_faces(
        0, field, X, 1, faces, faces_of(*fine_recv, 1), faces_of(*fine_recv, 2)
    )
    field = fine_sweep(field, outer_sum(sums, X, 1, faces))
    sums = outer_sum(fine_sums(field), X, 1, later_faces)
    coarse_rhs = [
        pooled([sums[c][x] - (6.0 + r_ref[x]) * field[c][x] for x in range(X)]) for c in range(C)
    ]
    correction = [[coarse_weight[x] * coarse_rhs[c][x] for x in range(Xc)] for c in range(C)]
    deep_send(1, correction, Xc, 2)
    for j in range(blocks):
        pl.when(me["gx"] != j)(c_copy(j, j).wait_recv)
    loads[3].wait()
    tiles_here = c_send.shape[1]
    first_tiles = (tiles_here + 1) // 2
    finish_compressed(range(first_tiles))

    def coarse_sweep(current, faces):
        total = outer_sum(inner_sum(current, Xc, 2), Xc, 2, faces)
        return [
            [keep * current[c][x] + first[c][x] + coarse_step[x] * total[c][x] for x in range(Xc)]
            for c in range(C)
        ]

    first = correction
    arrive(False, 0)
    step_faces = faces_of(*coarse_recv, 0)
    deep_arrive(1)
    first_faces = deep_faces(1)
    later_faces = advance_faces(1, correction, Xc, 2, first_faces, first_faces, step_faces)
    correction = coarse_sweep(coarse_sweep(correction, first_faces), later_faces)
    deep_send(2, correction, Xc, 2)
    finish_compressed(range(first_tiles, tiles_here))
    deep_arrive(2)
    faces = deep_faces(2)
    later_faces = advance_faces(2, correction, Xc, 2, faces, first_faces, step_faces)
    correction = coarse_sweep(correction, faces)
    spread = [[correction[c][x // 2] for x in range(X)] for c in range(C)]
    added = inner_sum(spread, X, 1)
    sums = [[sums[c][x] + added[c][x] for x in range(X)] for c in range(C)]
    sums = outer_sum(sums, X, 1, later_faces, repeat=2)
    for c in range(C):
        for x in range(X):
            vel_ref[c, x] = keep * (field[c][x] + spread[c][x]) + w_buf[x] * sums[c][x]

    for phase in range(SWEEPS + 1):
        sent(True, phase)
    sent(False, 0)
    for phase in range(1 + COARSE_SWEEPS // 2):
        deep_sent(phase)
    for j in range(blocks):
        pl.when(me["gx"] != j)(c_copy(j, me["gx"]).wait_send)


def on_device(counts, velocity_prev, forcing, reaction):
    C, X, Y, Z = velocity_prev.shape
    blocks = counts["gx"]
    kept = X // 2
    chunk = Z // blocks
    tiles = -(-(C * (Y // 8)) // (Z // chunk))
    matrix = jnp.asarray(finish_matrix(X, blocks, 8))
    vmem = pl.BlockSpec(memory_space=pltpu.VMEM)

    def buffers(phases, width):
        return [
            pltpu.VMEM((phases, 2, C, Y, Z), jnp.float32),
            pltpu.VMEM((phases, 2, C, Y, Z), jnp.float32),
            pltpu.VMEM((phases, 2, -(-C * width // 8) * 8, Z), jnp.float32),
            pltpu.VMEM((phases, 2, -(-C * width // 8) * 8, Z), jnp.float32),
            pltpu.VMEM((phases, Y, Z), jnp.float32),
            pltpu.VMEM((phases, 2, Y, Z), jnp.float32),
        ]

    def deep_buffers(phases, width):
        rows = -(-C * width // 8) * 8
        return [
            pltpu.VMEM((phases, 2, 2, C, Y, Z), jnp.float32),
            pltpu.VMEM((phases, 2, 2, C, Y, Z), jnp.float32),
            pltpu.VMEM((phases, 2, 2, rows, Z), jnp.float32),
            pltpu.VMEM((phases, 2, 2, rows, Z), jnp.float32),
            pltpu.VMEM((phases, Y, Z), jnp.float32),
            pltpu.VMEM((phases, 2, Y, Z), jnp.float32),
            pltpu.VMEM((phases, 4, rows, Z), jnp.float32),
            pltpu.VMEM((phases, 4, Y, Z), jnp.float32),
            pltpu.VMEM((phases, 4, Y, Z), jnp.float32),
        ]

    phases = SWEEPS + 2
    velocity, compressed = pl.pallas_call(
        functools.partial(kernel, counts),
        out_shape=(
            jax.ShapeDtypeStruct((C, X, Y, Z), jnp.float32),
            jax.ShapeDtypeStruct((C, Y, kept * blocks, chunk), jnp.float32),
        ),
        in_specs=[pl.BlockSpec(memory_space=pltpu.HBM)] * 4,
        out_specs=(vmem, vmem),
        scratch_shapes=[
            pltpu.VMEM((C, X, Y, Z), jnp.float32),
            pltpu.VMEM((C, X, Y, Z), jnp.float32),
            pltpu.VMEM((X, Y, Z), jnp.float32),
            pltpu.VMEM(matrix.shape, jnp.float32),
        ] + buffers(SWEEPS + 1, X) + buffers(1, X // 2) + deep_buffers(1 + COARSE_SWEEPS // 2, X) + [
            pltpu.VMEM((blocks, tiles, kept, 8, Z), jnp.float32),
            pltpu.VMEM((blocks, tiles, kept, 8, Z), jnp.float32),
            pltpu.VMEM((X, Y, Z), jnp.float32),
            pltpu.SemaphoreType.DMA((phases, 6)),
            pltpu.SemaphoreType.DMA((phases, 6)),
            pltpu.SemaphoreType.DMA((1 + COARSE_SWEEPS // 2, 18)),
            pltpu.SemaphoreType.DMA((1 + COARSE_SWEEPS // 2, 18)),
            pltpu.SemaphoreType.DMA((blocks,)),
            pltpu.SemaphoreType.DMA((blocks,)),
            pltpu.SemaphoreType.DMA((4,)),
        ],
        compiler_params=pltpu.CompilerParams(collective_id=0, has_side_effects=True, vmem_limit_bytes=40000000),
    )(*(pltpu.with_memory_space_constraint(a, pltpu.HBM) for a in (velocity_prev, forcing, reaction, matrix)))
    return velocity, jnp.swapaxes(compressed, 2, 3)


def solution(mesh):
    counts = {axis: mesh.shape[axis] for axis in ("agg", "gx", "gy")}
    placed = (P(None, "gx", "gy", "agg"), P(None, "gx", "gy", "agg"), P("gx", "gy", "agg"))
    return jax.shard_map(
        functools.partial(on_device, counts),
        mesh=mesh,
        in_specs=placed,
        out_specs=(P(None, "gx", "gy", "agg"), P(None, "gy", ("agg", "gx"), None)),
        check_vma=False,
    )
```

```python
import functools

import jax
import jax.numpy as jnp
import numpy as np
from jax import lax
from jax.experimental import pallas as pl
from jax.experimental.pallas import tpu as pltpu
from jax.sharding import PartitionSpec as P

SWEEPS = 2
COARSE_SWEEPS = 4
LX = 5
MESH = pl.DeviceIdType.MESH

damping = 0.8
keep = 1.0 - damping
root_half = 0.7071067811865476


def local_levels(cells_x):
    return min(LX, cells_x.bit_length() - 1)


def finish_matrix(cells_x, blocks, rows):
    levels = local_levels(cells_x)
    kept = cells_x // 2
    eye = np.eye(blocks * kept).reshape(blocks, kept, blocks * kept)
    width = cells_x >> levels
    approx = eye[:, :width].reshape(blocks * width, -1)
    details, at = [], width
    for level in range(levels, 1, -1):
        width = cells_x >> level
        details.append(eye[:, at : at + width].reshape(blocks * width, -1))
        at += width
    for level in range(levels, LX):
        low, high = approx[0::2], approx[1::2]
        approx, detail = (low + high) * root_half, (low - high) * root_half
        details.insert(0, detail)
    along_x = np.concatenate([approx] + details, axis=0)
    along_y = np.zeros((rows, rows))
    for row in range(0, rows, 2):
        along_y[row, row : row + 2] = root_half
        along_y[row + 1, row : row + 2] = root_half, -root_half
    return np.einsum("qk,yr->yqkr", along_x, along_y).reshape(-1, blocks * kept * rows).astype(np.float32)


def neighbour_sides():
    return [(axis, high) for axis in ("gx", "gy", "agg") for high in (False, True)]


def edge_sides():
    pairs = (("gx", "gy"), ("gx", "agg"), ("gy", "agg"))
    return [((a, p), (b, q)) for a, b in pairs for p in (False, True) for q in (False, True)]


def kernel(
    sizes, v_hbm, f_hbm, r_hbm, m_hbm, vel_ref, comp_ref, v_ref, f_ref, r_ref, m_ref,
    xs_fine, xr_fine, ys_fine, yr_fine, zs_fine, zr_fine,
    xs_coarse, xr_coarse, ys_coarse, yr_coarse, zs_coarse, zr_coarse,
    xs_deep, xr_deep, ys_deep, yr_deep, zs_deep, zr_deep, exy, exz, eyz,
c_send, c_recv, w_buf, send_sem, recv_sem, deep_send_sem, deep_recv_sem, c_send_sem, c_recv_sem, in_sem,
):
    counts = sizes
    C, X, Y, Z = v_ref.shape
    Xc = X // 2
    half = Z // 2
    me = {axis: lax.axis_index(axis) for axis in counts}
    blocks = counts["gx"]
    chunk = Z // blocks

    def exists(axis, high):
        return me[axis] < counts[axis] - 1 if high else me[axis] > 0

    loads = [
        pltpu.make_async_copy(src, dst, in_sem.at[i])
        for i, (src, dst) in enumerate(
            ((v_hbm, v_ref), (f_hbm, f_ref), (r_hbm, r_ref), (m_hbm, m_ref))
        )
    ]
    for load in loads:
        load.start()
    def beside(*sides):
        return {axis: me[axis] + (1 if high else -1) for axis, high in sides}

    barrier = pltpu.get_barrier_semaphore()
    expected = blocks - 1
    for step in range(1, blocks):
        pl.semaphore_signal(
            barrier, inc=1, device_id={"gx": lax.rem(me["gx"] + step, blocks)}, device_id_type=MESH
        )
    for axis, high in neighbour_sides()[2:]:
        there = exists(axis, high)
        expected = expected + there.astype(jnp.int32)

        @pl.when(there)
        def _():
            pl.semaphore_signal(
                barrier, inc=1, device_id={axis: me[axis] + (1 if high else -1)}, device_id_type=MESH
            )

    for (axis_a, high_a), (axis_b, high_b) in edge_sides():
        there = exists(axis_a, high_a) & exists(axis_b, high_b)
        expected = expected + there.astype(jnp.int32)

        @pl.when(there)
        def _():
            pl.semaphore_signal(
                barrier, inc=1, device_id=beside((axis_a, high_a), (axis_b, high_b)), device_id_type=MESH
            )

    received = {
        "gx": (xr_fine, xr_coarse, xr_deep),
        "gy": (yr_fine, yr_coarse, yr_deep),
        "agg": (zr_fine, zr_coarse, zr_deep),
    }
    edges = {("gx", "gy"): exy, ("gx", "agg"): exz, ("gy", "agg"): eyz}
    for (axis_a, high_a), (axis_b, high_b) in edge_sides():
        @pl.when(jnp.logical_not(exists(axis_a, high_a) & exists(axis_b, high_b)))
        def _():
            buffer = edges[axis_a, axis_b]
            for phase in range(buffer.shape[0]):
                buffer[phase, 2 * int(high_a) + int(high_b)] = jnp.zeros(buffer.shape[2:], buffer.dtype)

    for buffer in (ys_coarse, ys_deep):
        buffer[...] = jnp.zeros(buffer.shape, buffer.dtype)
    for axis, high in neighbour_sides():
        @pl.when(jnp.logical_not(exists(axis, high)))
        def _():
            for buffer in received[axis]:
                for phase in range(buffer.shape[0]):
                    buffer[phase, int(high)] = jnp.zeros(buffer.shape[2:], buffer.dtype)

    row = lax.broadcasted_iota(jnp.int32, (Y, Z), 0)
    lane = lax.broadcasted_iota(jnp.int32, (Y, Z), 1)
    zero = jnp.zeros((Y, Z), jnp.float32)

    def pack(fields, width, phase, xs, ys, zs):
        packed = zero
        for c in range(C):
            for x in range(width):
                k = c * width + x
                field = fields[c][x]
                ys[phase, 0, k : k + 1] = field[0:1]
                ys[phase, 1, k : k + 1] = field[Y - 1 : Y]
                packed = jnp.where(lane == k, field[:, 0:1], packed)
                packed = jnp.where(lane == half + k, field[:, Z - 1 : Z], packed)
        zs[phase] = packed

    def copies(fine, phase):
        number = phase if fine else SWEEPS + 1 + phase
        xs, xr, ys, yr, zs, zr = (
            (xs_fine, xr_fine, ys_fine, yr_fine, zs_fine, zr_fine)
            if fine
            else (xs_coarse, xr_coarse, ys_coarse, yr_coarse, zs_coarse, zr_coarse)
        )
        made = []
        for slot, (axis, high) in enumerate(neighbour_sides()):
            side = int(high)
            if axis == "gx":
                if fine and phase == 0:
                    src = v_ref.at[:, X - 1 if high else 0]
                else:
                    src = xs.at[phase, side]
                dst = xr.at[phase, 1 - side]
            elif axis == "gy":
                src, dst = ys.at[phase, side], yr.at[phase, 1 - side]
            else:
                src, dst = zs.at[phase], zr.at[phase, 1 - side]
            made.append((
                axis,
                high,
                pltpu.make_async_remote_copy(
                    src_ref=src,
                    dst_ref=dst,
                    send_sem=send_sem.at[number, slot],
                    recv_sem=recv_sem.at[number, slot],
                    device_id={axis: me[axis] + (1 if high else -1)},
                    device_id_type=MESH,
                ),
            ))
        return made

    def start(fine, phase, axes=("gx", "gy", "agg")):
        for axis, high, copy in copies(fine, phase):
            if axis in axes:
                pl.when(exists(axis, high))(copy.start)

    def send(fine, phase, fields, width):
        xs, ys, zs = fine_send if fine else coarse_send
        for c in range(C):
            xs[phase, 0, c] = fields[c][0]
            xs[phase, 1, c] = fields[c][width - 1]
        start(fine, phase, ("gx",))
        pack(fields, width, phase, xs, ys, zs)
        start(fine, phase, ("gy", "agg"))

    def arrive(fine, phase):
        for axis, high, copy in copies(fine, phase):
            pl.when(exists(axis, not high))(copy.wait_recv)

    def sent(fine, phase):
        for axis, high, copy in copies(fine, phase):
            pl.when(exists(axis, high))(copy.wait_send)

    def inner_sum(fields, width, stride):
        sums = []
        for c in range(C):
            line = []
            for x in range(width):
                field = fields[c][x]
                total = jnp.where(row < stride, zero, pltpu.roll(field, stride, 0))
                total = total + jnp.where(row >= Y - stride, zero, pltpu.roll(field, Y - stride, 0))
                total = total + jnp.where(lane < stride, zero, pltpu.roll(field, stride, 1))
                total = total + jnp.where(lane >= Z - stride, zero, pltpu.roll(field, Z - stride, 1))
                if x > 0:
                    total = total + fields[c][x - 1]
                if x < width - 1:
                    total = total + fields[c][x + 1]
                line.append(total)
            sums.append(line)
        return sums

    def outer_sum(sums, width, stride, faces, repeat=1):
        along_x, along_y, along_z = faces
        result = []
        for c in range(C):
            line = []
            for x in range(width):
                k = c * (width // repeat) + x // repeat
                total = sums[c][x]
                total = total + jnp.where(row < stride, along_y[0][k : k + 1], 0.0)
                total = total + jnp.where(row >= Y - stride, along_y[1][k : k + 1], 0.0)
                total = total + jnp.where(lane < stride, along_z[0][:, k : k + 1], 0.0)
                total = total + jnp.where(lane >= Z - stride, along_z[1][:, k : k + 1], 0.0)
                if x == 0:
                    total = total + along_x[0][c]
                if x == width - 1:
                    total = total + along_x[1][c]
                line.append(total)
            result.append(line)
        return result

    def faces_of(xr, yr, zr, phase):
        return (
            [[xr[phase, side, c] for c in range(C)] for side in range(2)],
            [yr[phase, side] for side in range(2)],
            [pltpu.roll(zr[phase, 0], half, 1), zr[phase, 1]],
        )

    group = Z // 4
    far = {0: 2, 1: 0}

    def rows_of(width):
        return -(-C * width // 8) * 8

    def deep_copies(phase):
        made = []
        rows = pl.ds(0, rows_of(X if phase == 0 else Xc))
        for slot, (first, second) in enumerate(edge_sides()):
            number = 2 * int(first[1]) + int(second[1])
            back = 3 - number
            if second[0] == "gy":
                src, dst = ys_deep.at[phase, int(second[1]), 0, rows], exy.at[phase, back, rows]
            else:
                src, dst = zs_deep.at[phase], (exz if first[0] == "gx" else eyz).at[phase, back]
            made.append(((first, second), src, dst, 6 + slot))
        for slot, (axis, high) in enumerate(neighbour_sides()):
            side = int(high)
            if axis == "gx":
                src, dst = xs_deep.at[phase, side], xr_deep.at[phase, 1 - side]
            elif axis == "gy":
                src, dst = ys_deep.at[phase, side, :, rows], yr_deep.at[phase, 1 - side, :, rows]
            else:
                src, dst = zs_deep.at[phase], zr_deep.at[phase, 1 - side]
            made.append((((axis, high),), src, dst, slot))
        return [
            (
                sides,
                pltpu.make_async_remote_copy(
                    src_ref=src,
                    dst_ref=dst,
                    send_sem=deep_send_sem.at[phase, slot],
                    recv_sem=deep_recv_sem.at[phase, slot],
                    device_id=beside(*sides),
                    device_id_type=MESH,
                ),
            )
            for sides, src, dst, slot in made
        ]

    def all_exist(sides, flip):
        there = None
        for axis, high in sides:
            one = exists(axis, high != flip)
            there = one if there is None else there & one
        return there

    def deep_send(phase, fields, width, stride):
        for c in range(C):
            for depth in range(2):
                xs_deep[phase, 0, depth, c] = fields[c][depth]
                xs_deep[phase, 1, depth, c] = fields[c][width - 1 - depth]
        ready = deep_copies(phase)
        packed = zero
        for c in range(C):
            for x in range(width):
                k = c * width + x
                field = fields[c][x]
                for depth in range(2):
                    at = depth * stride
                    ys_deep[phase, 0, depth, k : k + 1] = field[at : at + 1]
                    ys_deep[phase, 1, depth, k : k + 1] = field[Y - 1 - at : Y - at]
                    packed = jnp.where(lane == depth * group + k, field[:, at : at + 1], packed)
                    packed = jnp.where(
                        lane == (2 + depth) * group + k, field[:, Z - 1 - at : Z - at], packed
                    )
        zs_deep[phase] = packed
        for sides, copy in ready:
            pl.when(all_exist(sides, False))(copy.start)

    def deep_arrive(phase):
        for sides, copy in deep_copies(phase):
            pl.when(all_exist(sides, True))(copy.wait_recv)

    def deep_sent(phase):
        for sides, copy in deep_copies(phase):
            pl.when(all_exist(sides, False))(copy.wait_send)

    def lanes_from(packed, number, shift=0):
        turn = (shift - number * group) % Z
        return pltpu.roll(packed, turn, 1) if turn else packed

    def deep_faces(phase):
        return (
            [[xr_deep[phase, side, 0, c] for c in range(C)] for side in range(2)],
            [yr_deep[phase, side, 0, : rows_of(X if phase == 0 else Xc)] for side in range(2)],
            [lanes_from(zr_deep[phase, side], far[side]) for side in range(2)],
        )

    def advance_faces(phase, fields, width, stride, faces, added, weight):
        along_x, along_y, along_z = [], [], []
        rows = rows_of(width)
        k_row = lax.broadcasted_iota(jnp.int32, (rows, Z), 0)
        k_lane = lax.broadcasted_iota(jnp.int32, (rows, Z), 1)
        for side in range(2):
            near = width - 1 if side == 0 else 0
            planes = []
            for c in range(C):
                plane = faces[0][side][c]
                k = c * width + near
                total = xr_deep[phase, side, 1, c] + fields[c][0 if side == 0 else width - 1]
                total = total + jnp.where(
                    row < stride, exy[phase, 2 * side, k : k + 1], pltpu.roll(plane, stride, 0)
                )
                total = total + jnp.where(
                    row >= Y - stride, exy[phase, 2 * side + 1, k : k + 1], pltpu.roll(plane, Y - stride, 0)
                )
                low = exz[phase, 2 * side][:, far[0] * group + k : far[0] * group + k + 1]
                high = exz[phase, 2 * side + 1][:, far[1] * group + k : far[1] * group + k + 1]
                total = total + jnp.where(lane < stride, low, pltpu.roll(plane, stride, 1))
                total = total + jnp.where(lane >= Z - stride, high, pltpu.roll(plane, Z - stride, 1))
                planes.append(keep * plane + added[0][side][c] + weight[0][side][c] * total)
            along_x.append(planes)

            layer = faces[1][side]
            total = yr_deep[phase, side, 1, :rows] + ys_deep[phase, side, 0, :rows]
            spot = k_row % width
            total = total + jnp.where(
                spot == 0, pltpu.roll(exy[phase, side, :rows], rows - (width - 1), 0), pltpu.roll(layer, 1, 0)
            )
            total = total + jnp.where(
                spot == width - 1, pltpu.roll(exy[phase, 2 + side, :rows], width - 1, 0), pltpu.roll(layer, rows - 1, 0)
            )
            at = Y - 1 if side == 0 else 0
            ends = []
            for z_side in range(2):
                line = eyz[phase, 2 * side + z_side, at : at + 1]
                chosen = jnp.where(k_lane == far[z_side] * group + k_row, line, 0.0)
                ends.append(jnp.sum(chosen, axis=1, keepdims=True))
            total = total + jnp.where(k_lane < stride, ends[0], pltpu.roll(layer, stride, 1))
            total = total + jnp.where(k_lane >= Z - stride, ends[1], pltpu.roll(layer, Z - stride, 1))
            along_y.append(keep * layer + added[1][side] + weight[1][side] * total)

            layer = faces[2][side]
            total = lanes_from(zr_deep[phase, side], far[side] + 1)
            total = total + lanes_from(zs_deep[phase], 2 - far[side])
            low = lanes_from(eyz[phase, side], far[side])[Y - 1 : Y]
            high = lanes_from(eyz[phase, 2 + side], far[side])[0:1]
            total = total + jnp.where(row < stride, low, pltpu.roll(layer, stride, 0))
            total = total + jnp.where(row >= Y - stride, high, pltpu.roll(layer, Y - stride, 0))
            spot = lane % width
            total = total + jnp.where(
                spot == 0, lanes_from(exz[phase, side], far[side], 1 - width), pltpu.roll(layer, 1, 1)
            )
            total = total + jnp.where(
                spot == width - 1, lanes_from(exz[phase, 2 + side], far[side], width - 1), pltpu.roll(layer, Z - 1, 1)
            )
            along_z.append(keep * layer + added[2][side] + weight[2][side] * total)
        return along_x, along_y, along_z

    fine_recv = (xr_fine, yr_fine, zr_fine)
    coarse_recv = (xr_coarse, yr_coarse, zr_coarse)
    fine_send = (xs_fine, ys_fine, zs_fine)
    coarse_send = (xs_coarse, ys_coarse, zs_coarse)

    loads[0].wait()
    previous = [[v_ref[c, x] for x in range(X)] for c in range(C)]
    pack(previous, X, 0, *fine_send)
    pl.semaphore_wait(barrier, expected)
    start(True, 0)

    loads[1].wait()
    loads[2].wait()
    for x in range(X):
        w_buf[x] = damping / (6.0 + r_ref[x])
    scaled = [[w_buf[x] * f_ref[c, x] for x in range(X)] for c in range(C)]
    send(True, 1, scaled, X)
    send(True, 2, [[w_buf[x] for x in range(X)]] * C, X)

    kept = X // 2
    parts = Y // 8
    even_row = row % 2 == 0
    even_lane = lane % 2 == 0
    combos_per_tile = Z // chunk
    def c_copy(j, source):
        return pltpu.make_async_remote_copy(
            src_ref=c_send.at[j],
            dst_ref=c_recv.at[source],
            send_sem=c_send_sem.at[j],
            recv_sem=c_recv_sem.at[source],
            device_id={"gx": j},
            device_id_type=MESH,
        )

    def finish_compressed(tiles):
        coefs = blocks * kept
        for tile in tiles:
            gathered = c_recv[:, tile].reshape(coefs * 8, Z)
            done = lax.dot_general(
                m_ref[...], gathered, (((1,), (0,)), ((), ())),
                precision=lax.Precision.HIGHEST, preferred_element_type=jnp.float32,
            )
            for place in range(combos_per_tile):
                c, part = divmod(tile * combos_per_tile + place, parts)
                if c < C:
                    for y in range(8):
                        comp_ref[c, part * 8 + y] = done[
                            y * coefs : (y + 1) * coefs, place * chunk : (place + 1) * chunk
                        ]

    def pooled(planes):
        out = []
        for x in range(0, len(planes), 2):
            total = planes[x] + planes[x + 1]
            total = total + jnp.where(even_row, pltpu.roll(total, Y - 1, 0), pltpu.roll(total, 1, 0))
            total = total + jnp.where(even_lane, pltpu.roll(total, Z - 1, 1), pltpu.roll(total, 1, 1))
            out.append(total * 0.125)
        return out

    coarse_weight = [damping / ((6.0 + 4.0 * mean) * 0.25) for mean in pooled([r_ref[x] for x in range(X)])]
    coarse_step = [0.25 * weight for weight in coarse_weight]

    def fine_sums(current):
        inner = inner_sum(current, X, 1)
        return [[inner[c][x] + f_ref[c, x] for x in range(X)] for c in range(C)]

    def fine_sweep(current, total):
        return [[keep * current[c][x] + w_buf[x] * total[c][x] for x in range(X)] for c in range(C)]

    sums = fine_sums(previous)
    arrive(True, 0)
    field = fine_sweep(previous, outer_sum(sums, X, 1, faces_of(*fine_recv, 0)))
    deep_send(0, field, X, 1)
    send(False, 0, [coarse_step] * C, Xc)

    levels = local_levels(X)
    coefficients = []
    for c in range(C):
        approx, details = previous[c], []
        for level in range(levels):
            low, high = approx[0::2], approx[1::2]
            approx = [(a + b) * root_half for a, b in zip(low, high)]
            if level > 0:
                details = [(a - b) * root_half for a, b in zip(low, high)] + details
        line = []
        for values in approx + details:
            swapped = jnp.where(even_lane, pltpu.roll(values, Z - 1, 1), pltpu.roll(values, 1, 1))
            line.append((jnp.where(even_lane, values, -values) + swapped) * root_half)
        coefficients.append(line)
    row8 = lax.broadcasted_iota(jnp.int32, (8, Z), 1)
    for j in range(blocks):
        for k in range(kept):
            tiles = {}
            for c in range(C):
                for part in range(parts):
                    tile, place = divmod(c * parts + part, combos_per_tile)
                    values = coefficients[c][k][part * 8 : part * 8 + 8]
                    shift = (place * chunk - j * chunk) % Z
                    moved = pltpu.roll(values, shift, 1) if shift else values
                    if tile in tiles:
                        moved = jnp.where((row8 >= place * chunk) & (row8 < (place + 1) * chunk), moved, tiles[tile])
                    tiles[tile] = moved
            for tile, value in tiles.items():
                c_send[j, tile, k] = value

    for j in range(blocks):
        pl.when(me["gx"] != j)(c_copy(j, me["gx"]).start)

        @pl.when(me["gx"] == j)
        def _():
            c_recv[j] = c_send[j]

    sums = fine_sums(field)
    arrive(True, 1)
    arrive(True, 2)
    deep_arrive(0)
    faces = deep_faces(0)
    later_faces = advance_faces(
        0, field, X, 1, faces, faces_of(*fine_recv, 1), faces_of(*fine_recv, 2)
    )
    field = fine_sweep(field, outer_sum(sums, X, 1, faces))
    sums = outer_sum(fine_sums(field), X, 1, later_faces)
    coarse_rhs = [
        pooled([sums[c][x] - (6.0 + r_ref[x]) * field[c][x] for x in range(X)]) for c in range(C)
    ]
    correction = [[coarse_weight[x] * coarse_rhs[c][x] for x in range(Xc)] for c in range(C)]
    deep_send(1, correction, Xc, 2)
    for j in range(blocks):
        pl.when(me["gx"] != j)(c_copy(j, j).wait_recv)
    loads[3].wait()
    tiles_here = c_send.shape[1]
    first_tiles = (tiles_here + 1) // 2
    finish_compressed(range(first_tiles))

    def coarse_sweep(current, faces):
        total = outer_sum(inner_sum(current, Xc, 2), Xc, 2, faces)
        return [
            [keep * current[c][x] + first[c][x] + coarse_step[x] * total[c][x] for x in range(Xc)]
            for c in range(C)
        ]

    first = correction
    arrive(False, 0)
    step_faces = faces_of(*coarse_recv, 0)
    deep_arrive(1)
    first_faces = deep_faces(1)
    later_faces = advance_faces(1, correction, Xc, 2, first_faces, first_faces, step_faces)
    correction = coarse_sweep(coarse_sweep(correction, first_faces), later_faces)
    deep_send(2, correction, Xc, 2)
    finish_compressed(range(first_tiles, tiles_here))
    deep_arrive(2)
    faces = deep_faces(2)
    later_faces = advance_faces(2, correction, Xc, 2, faces, first_faces, step_faces)
    correction = coarse_sweep(correction, faces)
    spread = [[correction[c][x // 2] for x in range(X)] for c in range(C)]
    added = inner_sum(spread, X, 1)
    sums = [[sums[c][x] + added[c][x] for x in range(X)] for c in range(C)]
    sums = outer_sum(sums, X, 1, later_faces, repeat=2)
    for c in range(C):
        for x in range(X):
            vel_ref[c, x] = keep * (field[c][x] + spread[c][x]) + w_buf[x] * sums[c][x]

    for phase in range(SWEEPS + 1):
        sent(True, phase)
    sent(False, 0)
    for phase in range(1 + COARSE_SWEEPS // 2):
        deep_sent(phase)
    for j in range(blocks):
        pl.when(me["gx"] != j)(c_copy(j, me["gx"]).wait_send)


def on_device(counts, velocity_prev, forcing, reaction):
    C, X, Y, Z = velocity_prev.shape
    blocks = counts["gx"]
    kept = X // 2
    chunk = Z // blocks
    tiles = -(-(C * (Y // 8)) // (Z // chunk))
    matrix = jnp.asarray(finish_matrix(X, blocks, 8))
    vmem = pl.BlockSpec(memory_space=pltpu.VMEM)

    def buffers(phases, width):
        return [
            pltpu.VMEM((phases, 2, C, Y, Z), jnp.float32),
            pltpu.VMEM((phases, 2, C, Y, Z), jnp.float32),
            pltpu.VMEM((phases, 2, -(-C * width // 8) * 8, Z), jnp.float32),
            pltpu.VMEM((phases, 2, -(-C * width // 8) * 8, Z), jnp.float32),
            pltpu.VMEM((phases, Y, Z), jnp.float32),
            pltpu.VMEM((phases, 2, Y, Z), jnp.float32),
        ]

    def deep_buffers(phases, width):
        rows = -(-C * width // 8) * 8
        return [
            pltpu.VMEM((phases, 2, 2, C, Y, Z), jnp.float32),
            pltpu.VMEM((phases, 2, 2, C, Y, Z), jnp.float32),
            pltpu.VMEM((phases, 2, 2, rows, Z), jnp.float32),
            pltpu.VMEM((phases, 2, 2, rows, Z), jnp.float32),
            pltpu.VMEM((phases, Y, Z), jnp.float32),
            pltpu.VMEM((phases, 2, Y, Z), jnp.float32),
            pltpu.VMEM((phases, 4, rows, Z), jnp.float32),
            pltpu.VMEM((phases, 4, Y, Z), jnp.float32),
            pltpu.VMEM((phases, 4, Y, Z), jnp.float32),
        ]

    phases = SWEEPS + 2
    velocity, compressed = pl.pallas_call(
        functools.partial(kernel, counts),
        out_shape=(
            jax.ShapeDtypeStruct((C, X, Y, Z), jnp.float32),
            jax.ShapeDtypeStruct((C, Y, kept * blocks, chunk), jnp.float32),
        ),
        in_specs=[pl.BlockSpec(memory_space=pltpu.HBM)] * 4,
        out_specs=(vmem, vmem),
        scratch_shapes=[
            pltpu.VMEM((C, X, Y, Z), jnp.float32),
            pltpu.VMEM((C, X, Y, Z), jnp.float32),
            pltpu.VMEM((X, Y, Z), jnp.float32),
            pltpu.VMEM(matrix.shape, jnp.float32),
        ] + buffers(SWEEPS + 1, X) + buffers(1, X // 2) + deep_buffers(1 + COARSE_SWEEPS // 2, X) + [
            pltpu.VMEM((blocks, tiles, kept, 8, Z), jnp.float32),
            pltpu.VMEM((blocks, tiles, kept, 8, Z), jnp.float32),
            pltpu.VMEM((X, Y, Z), jnp.float32),
            pltpu.SemaphoreType.DMA((phases, 6)),
            pltpu.SemaphoreType.DMA((phases, 6)),
            pltpu.SemaphoreType.DMA((1 + COARSE_SWEEPS // 2, 18)),
            pltpu.SemaphoreType.DMA((1 + COARSE_SWEEPS // 2, 18)),
            pltpu.SemaphoreType.DMA((blocks,)),
            pltpu.SemaphoreType.DMA((blocks,)),
            pltpu.SemaphoreType.DMA((4,)),
        ],
        compiler_params=pltpu.CompilerParams(collective_id=0, has_side_effects=True, vmem_limit_bytes=40000000),
    )(*(pltpu.with_memory_space_constraint(a, pltpu.HBM) for a in (velocity_prev, forcing, reaction, matrix)))
    return velocity, jnp.swapaxes(compressed, 2, 3)


def solution(mesh):
    counts = {axis: mesh.shape[axis] for axis in ("agg", "gx", "gy")}
    placed = (P(None, "gx", "gy", "agg"), P(None, "gx", "gy", "agg"), P("gx", "gy", "agg"))
    return jax.shard_map(
        functools.partial(on_device, counts),
        mesh=mesh,
        in_specs=placed,
        out_specs=(P(None, "gx", "gy", "agg"), P(None, "gy", ("agg", "gx"), None)),
        check_vma=False,
    )
```
